128 devices in a mesh: dp: 1, sp: 128 (over z, y, x, core).
Axes of the slice: x: 4, y: 4, z: 4, core: 2. Of those that a mesh axis runs over, the one named last changes fastest.
Arguments:
- hidden: bfloat16 [2048, 5120], P(('dp', 'sp'))
- seg_ids: int32 [2048], P(('dp', 'sp'))
- positions: int32 [2048], P(('dp', 'sp'))
- prefix_lat: bfloat16 [2048, 576], P(('dp', 'sp'))
- prefix_seg: int32 [2048], P(('dp', 'sp'))
- w_dq: bfloat16 [5120, 1536], replicated
- gain_q: bfloat16 [1536], replicated
- w_uq: bfloat16 [1536, 24576], replicated
- w_dkv: bfloat16 [5120, 576], replicated
- gain_kv: bfloat16 [512], replicated
- w_ukv: bfloat16 [512, 32768], replicated
- w_o: bfloat16 [16384, 5120], replicated
Outputs:
- output: bfloat16 [2048, 5120], P(('dp', 'sp'))
All inputs are finite; a program needn't handle non-finite values.
Results may differ from the reference program's by a relative error of at most 0.00583197.
Values are sent between devices in bfloat16 or wider.
A program may use at most 1.25 GiB of HBM per device.

```python
import jax
import jax.numpy as jnp
from jax import lax

D = 5120
HEADS = 128
QLAT = 1536
TOKENS = 2048
PREFIX = 2048
PROMPTS = 2
KV_LAT = 512
ROPE_DIM = 64
NOPE_DIM = 128
V_DIM = 128
QK_DIM = NOPE_DIM + ROPE_DIM
KV_HEAD = NOPE_DIM + V_DIM
LAT_DIM = KV_LAT + ROPE_DIM
QBLK = min(TOKENS, max(1, 2048 // HEADS))
OUT_GAIN = 0.6 * ((2 * PREFIX + TOKENS) // (2 * PROMPTS)) ** 0.5
EPS = 1e-6
ROPE_BASE = 10000.0
NEG_BIG = -1e30


def packed_layout(key, total):
    cuts = jnp.sort(jax.random.permutation(key, total - 1)[: PROMPTS - 1] + 1).astype(jnp.int32)
    row_idx = jnp.arange(total, dtype=jnp.int32)
    prompt_ids = jnp.sum((row_idx[:, None] >= cuts[None, :]).astype(jnp.int32), axis=1)
    starts = jnp.concatenate([jnp.zeros((1,), jnp.int32), cuts])
    ends = jnp.concatenate([cuts, jnp.full((1,), total, jnp.int32)])
    offsets = row_idx - starts[prompt_ids]
    return prompt_ids, offsets, ends - starts


def setup_inputs(seed: int = 0, part: int = 0) -> dict:
    part_key = jax.random.fold_in(jax.random.key(seed), part)
    key_hid, key_new, key_pre, key_lat = jax.random.split(part_key, 4)
    weight_keys = jax.random.split(jax.random.key(seed + 1), 7)
    new_layout = packed_layout(key_new, TOKENS)
    pre_layout = packed_layout(key_pre, PREFIX)
    seg_ids = new_layout[0]
    positions = pre_layout[2][seg_ids] + new_layout[1]
    hidden = jax.random.normal(key_hid, (TOKENS, D), jnp.float32)
    prefix_lat = jax.random.normal(key_lat, (PREFIX, LAT_DIM), jnp.float32)
    w_dq = jax.random.normal(weight_keys[0], (D, QLAT), jnp.float32) * D ** -0.5
    gain_q = 1.0 + 0.3 * jax.random.normal(weight_keys[1], (QLAT,), jnp.float32)
    w_uq = jax.random.normal(weight_keys[2], (QLAT, HEADS * QK_DIM), jnp.float32) * QLAT ** -0.5
    w_dkv = jax.random.normal(weight_keys[3], (D, LAT_DIM), jnp.float32) * D ** -0.5
    gain_kv = 1.0 + 0.3 * jax.random.normal(weight_keys[4], (KV_LAT,), jnp.float32)
    w_ukv = jax.random.normal(weight_keys[5], (KV_LAT, HEADS * KV_HEAD), jnp.float32) * KV_LAT ** -0.5
    w_o = jax.random.normal(weight_keys[6], (HEADS * V_DIM, D), jnp.float32) * (HEADS * V_DIM) ** -0.5 * OUT_GAIN
    return {
        "hidden": hidden.astype(jnp.bfloat16),
        "seg_ids": seg_ids,
        "positions": positions,
        "prefix_lat": prefix_lat.astype(jnp.bfloat16),
        "prefix_seg": pre_layout[0],
        "w_dq": w_dq.astype(jnp.bfloat16),
        "gain_q": gain_q.astype(jnp.bfloat16),
        "w_uq": w_uq.astype(jnp.bfloat16),
        "w_dkv": w_dkv.astype(jnp.bfloat16),
        "gain_kv": gain_kv.astype(jnp.bfloat16),
        "w_ukv": w_ukv.astype(jnp.bfloat16),
        "w_o": w_o.astype(jnp.bfloat16),
    }


def rms_norm(values, gain):
    inv_rms = lax.rsqrt(jnp.mean(values * values, axis=-1, keepdims=True) + EPS)
    return values * inv_rms * gain.astype(jnp.float32)


def rope_tables(positions):
    half_dim = ROPE_DIM // 2
    inv_freq = ROPE_BASE ** (-jnp.arange(half_dim, dtype=jnp.float32) / half_dim)
    angles = positions.astype(jnp.float32)[:, None] * inv_freq[None, :]
    return jnp.cos(angles), jnp.sin(angles)


def rope_apply(values, cos_t, sin_t):
    half_dim = ROPE_DIM // 2
    lower_half = values[..., :half_dim]
    upper_half = values[..., half_dim:]
    return jnp.concatenate([lower_half * cos_t - upper_half * sin_t, upper_half * cos_t + lower_half * sin_t], axis=-1)


def reference(hidden, seg_ids, positions, prefix_lat, prefix_seg, w_dq, gain_q, w_uq, w_dkv, gain_kv, w_ukv, w_o):
    q_lat = rms_norm(jnp.dot(hidden, w_dq, preferred_element_type=jnp.float32), gain_q).astype(jnp.bfloat16)
    kv_down = jnp.dot(hidden, w_dkv, preferred_element_type=jnp.float32)
    cos_t, sin_t = rope_tables(positions)
    kv_lat = rms_norm(kv_down[:, :KV_LAT], gain_kv).astype(jnp.bfloat16)
    key_rope_new = rope_apply(kv_down[:, KV_LAT:], cos_t, sin_t).astype(jnp.bfloat16)
    key_lat = jnp.concatenate([prefix_lat, jnp.concatenate([kv_lat, key_rope_new], axis=1)], axis=0)
    key_seg = jnp.concatenate([prefix_seg, seg_ids])
    key_pos = jnp.concatenate([jnp.full((PREFIX,), -1, jnp.int32), positions])
    q_full = jnp.dot(q_lat, w_uq, preferred_element_type=jnp.float32).reshape(TOKENS, HEADS, QK_DIM)
    q_nope = q_full[..., :NOPE_DIM].astype(jnp.bfloat16)
    q_rope = rope_apply(q_full[..., NOPE_DIM:], cos_t[:, None, :], sin_t[:, None, :]).astype(jnp.bfloat16)
    kv_up = jnp.dot(key_lat[:, :KV_LAT], w_ukv, preferred_element_type=jnp.float32).astype(jnp.bfloat16)
    kv_up = kv_up.reshape(PREFIX + TOKENS, HEADS, KV_HEAD)
    k_nope = kv_up[..., :NOPE_DIM].astype(jnp.float32)
    v_heads = kv_up[..., NOPE_DIM:].astype(jnp.float32)
    k_rope = key_lat[:, KV_LAT:].astype(jnp.float32)
    n_blocks = TOKENS // QBLK

    def attend(block):
        qn_blk, qr_blk, seg_blk, pos_blk = block
        scores = jnp.einsum("qhd,khd->hqk", qn_blk.astype(jnp.float32), k_nope)
        scores = scores + jnp.einsum("qhd,kd->hqk", qr_blk.astype(jnp.float32), k_rope)
        allowed = (seg_blk[:, None] == key_seg[None, :]) & (key_pos[None, :] <= pos_blk[:, None])
        scores = jnp.where(allowed[None], scores * QK_DIM ** -0.5, NEG_BIG)
        probs = jax.nn.softmax(scores, axis=-1).astype(jnp.bfloat16).astype(jnp.float32)
        return jnp.einsum("hqk,khd->qhd", probs, v_heads).astype(jnp.bfloat16)

    heads_out = lax.map(attend, (q_nope.reshape(n_blocks, QBLK, HEADS, NOPE_DIM), q_rope.reshape(n_blocks, QBLK, HEADS, ROPE_DIM), seg_ids.reshape(n_blocks, QBLK), positions.reshape(n_blocks, QBLK)))
    return jnp.dot(heads_out.reshape(TOKENS, HEADS * V_DIM), w_o, preferred_element_type=jnp.float32).astype(jnp.bfloat16)
```

```python
import functools

import jax
import jax.numpy as jnp
from jax import lax
from jax.experimental import pallas as pl
from jax.experimental.pallas import tpu as pltpu
from jax.sharding import PartitionSpec as P

MESH = pl.DeviceIdType.MESH
KV_LAT = 512
ROPE_DIM = 64
NOPE_DIM = 128
V_DIM = 128
QK_DIM = NOPE_DIM + ROPE_DIM
KV_HEAD = NOPE_DIM + V_DIM
EPS = 1e-6
ROPE_BASE = 10000.0
NEG_BIG = -1e30
LOG2E = 1.4426950408889634
RING = 4
ROWS = 16
PLANE_TOKENS = 512
HEADS_DEV = 4
KV_WIDTH = 640
META = KV_LAT + ROPE_DIM
KEY_BLOCK = 512
W_SLOTS = 8
Q_CHUNKS = 8
KV_CHUNKS = 4


def place():
    me = lax.axis_index("sp")
    core = lax.rem(me, 2)
    x = lax.rem(me // 2, RING)
    y = lax.rem(me // 8, RING)
    z = me // 32
    return z, y, x, core


def index_of(z, y, x, core):
    return ((z * RING + y) * RING + x) * 2 + core


def greet(peers):
    barrier = pltpu.get_barrier_semaphore()
    for peer in peers:
        pl.semaphore_signal(barrier, inc=1, device_id={"sp": peer}, device_id_type=MESH)
    pl.semaphore_wait(barrier, len(peers))


class Stream:
    def __init__(self, slot, ref, axes, order, lanes, sems, first=None):
        self.slot, self.ref, self.axes, self.order, self.lanes, self.first = slot, ref, axes, order, lanes, first
        self.send_sem, self.recv_sem, self.swap_send, self.swap_recv = sems
        z, y, x, self.core = place()
        self.at = (z, y, x)
        self.sent = []

    def view(self, full, core, moved=None):
        index = []
        for axis in self.axes:
            if axis in full:
                index.append(pl.ds(0, RING))
            elif moved is not None and moved[0] == axis:
                index.append(moved[1])
            else:
                index.append(self.at[axis])
        return self.ref.at[tuple(index) + (core, slice(None), self.lanes)]

    def back(self, axis, off):
        return lax.rem(self.at[axis] + RING - off, RING)

    def copy(self, src, dst, send, recv, device):
        return pltpu.make_async_remote_copy(src_ref=src, dst_ref=dst, send_sem=send, recv_sem=recv, device_id={"sp": device}, device_id_type=MESH)

    def send(self, phase):
        axis = self.order[phase]
        for off in (1, 3, 2):
            to = list(self.at)
            to[axis] = lax.rem(self.at[axis] + off, RING)
            mine = self.view(self.order[:phase], self.core)
            src = self.first if phase == 0 and self.first is not None else mine
            c = self.copy(src, mine, self.send_sem.at[self.slot, phase, off - 1], self.recv_sem.at[self.slot, phase, off - 1], index_of(*to, self.core))
            c.start()
            self.sent.append(c)

    def wait(self, phase, off):
        axis = self.order[phase]
        got = self.view(self.order[:phase], self.core, (axis, self.back(axis, off)))
        self.copy(got, got, self.send_sem.at[self.slot, phase, off - 1], self.recv_sem.at[self.slot, phase, off - 1], index_of(*self.at, self.core)).wait_recv()

    def swap(self, off):
        axis = self.order[-1]
        part = self.view(self.order[:-1], self.core, (axis, self.back(axis, off)))
        c = self.copy(part, part, self.swap_send.at[self.slot, off], self.swap_recv.at[self.slot, off], index_of(*self.at, 1 - self.core))
        c.start()
        self.sent.append(c)

    def start(self):
        self.send(0)

    def step(self, phase):
        for off in (1, 3, 2):
            self.wait(phase - 1, off)
        self.send(phase)
        if phase == len(self.order) - 1:
            self.swap(0)

    def finish(self):
        for off in (1, 3, 2):
            self.wait(len(self.order) - 1, off)
            self.swap(off)

    def done(self):
        axis = self.order[-1]
        for off in (0, 1, 3, 2):
            part = self.view(self.order[:-1], 1 - self.core, (axis, self.back(axis, off)))
            self.copy(part, part, self.swap_send.at[self.slot, off], self.swap_recv.at[self.slot, off], index_of(*self.at, 1 - self.core)).wait_recv()
        for c in self.sent:
            c.wait_send()


def rms_norm(values, gain):
    inv_rms = lax.rsqrt(jnp.mean(values * values, axis=-1, keepdims=True) + EPS)
    return values * inv_rms * gain.astype(jnp.float32)


def turn(values, cos_sin):
    half = ROPE_DIM // 2
    swapped = jnp.concatenate([values[:, half:], values[:, :half]], axis=1)
    return values * cos_sin[:, :ROPE_DIM] + swapped * cos_sin[:, ROPE_DIM:]


def gather_kernel(
    hid, pre, meta, cs, gain_q, gain_kv, wdq_hbm, wdkv_hbm,
    kv_out, cq_out, cs_out, cnt_out,
    kv_buf, cq_buf, cs_buf, wq_buf, wkv_buf, wq_sem, wkv_sem, send_sem, recv_sem, swap_send, swap_recv, out_sem,
):
    z, y, x, core = place()
    depth = hid.shape[1]
    q_step, kv_step = depth // Q_CHUNKS, depth // KV_CHUNKS
    kv_loads = [pltpu.make_async_copy(wdkv_hbm.at[pl.ds(k * kv_step, kv_step)], wkv_buf.at[pl.ds(k * kv_step, kv_step)], wkv_sem.at[k]) for k in range(KV_CHUNKS)]
    q_loads = [pltpu.make_async_copy(wdq_hbm.at[pl.ds(k * q_step, q_step)], wq_buf.at[pl.ds(k * q_step, q_step)], wq_sem.at[k]) for k in range(Q_CHUNKS)]
    for c in kv_loads + q_loads:
        c.start()

    peers = [index_of(z, y, x, 1 - core)]
    for off in (1, 2, 3):
        peers.append(index_of(lax.rem(z + off, RING), y, x, core))
        peers.append(index_of(z, lax.rem(y + off, RING), x, core))
        peers.append(index_of(z, y, lax.rem(x + off, RING), core))
    greet(peers)

    sems = (send_sem, recv_sem, swap_send, swap_recv)
    lanes = (pl.ds(0, 256), pl.ds(256, 256), pl.ds(512, 128))
    orders = ((2, 1, 0), (1, 0, 2), (0, 2, 1))
    space = (0, 1, 2)
    plane = (1, 2)
    old = [Stream(i, kv_buf.at[0], space, orders[i], lanes[i], sems, pre.at[:, lanes[i]]) for i in range(3)]
    new = [Stream(3 + i, kv_buf.at[1], space, orders[i], lanes[i], sems) for i in range(3)]
    half = cq_buf.shape[-1] // 2
    lat = [Stream(6, cq_buf, plane, (2, 1), pl.ds(0, half), sems), Stream(7, cq_buf, plane, (1, 2), pl.ds(half, half), sems)]
    turns = [Stream(8, cs_buf, plane, (2, 1), pl.ds(0, 128), sems, cs)]

    for s in old + turns:
        s.start()
    kv_buf[0, z, y, x, core] = pre[...]
    cs_buf[y, x, core] = cs[...]

    down = jnp.zeros((ROWS, META), jnp.float32)
    for k in range(KV_CHUNKS):
        kv_loads[k].wait()
        part = pl.ds(k * kv_step, kv_step)
        down = down + jnp.dot(hid[:, part], wkv_buf[part, :], preferred_element_type=jnp.float32)
    kv_lat = rms_norm(down[:, :KV_LAT], gain_kv[...]).astype(jnp.bfloat16)
    key_rope = turn(down[:, KV_LAT:], cs[...]).astype(jnp.bfloat16)
    kv_buf[1, z, y, x, core] = jnp.concatenate([kv_lat, key_rope, meta[...]], axis=1)
    for s in old + turns:
        s.step(1)
    for s in new:
        s.start()

    q_lat = jnp.zeros((ROWS, wq_buf.shape[1]), jnp.float32)
    for k in range(Q_CHUNKS):
        q_loads[k].wait()
        part = pl.ds(k * q_step, q_step)
        q_lat = q_lat + jnp.dot(hid[:, part], wq_buf[part, :], preferred_element_type=jnp.float32)
        if k == Q_CHUNKS // 2 - 1:
            for s in old:
                s.step(2)
            for s in turns:
                s.finish()
            for s in new:
                s.step(1)
    cq_buf[y, x, core] = rms_norm(q_lat, gain_q[...]).astype(jnp.bfloat16)
    for s in lat:
        s.start()
    for s in new:
        s.step(2)
    for s in old:
        s.finish()
    for s in lat:
        s.step(1)

    def counts(sec):
        tail = kv_buf[sec, :, :, :, :, :, pl.ds(512, 128)].reshape(-1, 128).astype(jnp.float32)
        cnt_out[pl.ds(sec, 1), :] = jnp.sum(tail, axis=0, keepdims=True)

    outs = []
    for s in old + turns:
        s.done()
    outs.append(pltpu.make_async_copy(kv_buf.at[0], kv_out.at[0], out_sem.at[0]))
    outs.append(pltpu.make_async_copy(cs_buf, cs_out, out_sem.at[1]))
    for c in outs:
        c.start()
    counts(0)
    for s in new:
        s.finish()
    for s in new:
        s.done()
    outs.append(pltpu.make_async_copy(kv_buf.at[1], kv_out.at[1], out_sem.at[2]))
    outs[-1].start()
    counts(1)
    for s in lat:
        s.finish()
    for s in lat:
        s.done()
    outs.append(pltpu.make_async_copy(cq_buf, cq_out, out_sem.at[3]))
    outs[-1].start()
    for c in outs:
        c.wait()


def gather_latents(hidden, pre, meta, cs, gain_q, gain_kv, w_dq, w_dkv):
    depth, q_width = w_dq.shape
    kv_shape = (2, RING, RING, RING, 2, ROWS, KV_WIDTH)
    cq_shape = (RING, RING, 2, ROWS, q_width)
    cs_shape = (RING, RING, 2, ROWS, 128)
    vmem = pl.BlockSpec(memory_space=pltpu.VMEM)
    hbm = pl.BlockSpec(memory_space=pl.ANY)
    return pl.pallas_call(
        gather_kernel,
        name="gather_latents",
        out_shape=(
            jax.ShapeDtypeStruct(kv_shape, jnp.bfloat16),
            jax.ShapeDtypeStruct(cq_shape, jnp.bfloat16),
            jax.ShapeDtypeStruct(cs_shape, jnp.float32),
            jax.ShapeDtypeStruct((2, 128), jnp.float32),
        ),
        in_specs=[vmem] * 6 + [hbm] * 2,
        out_specs=(hbm, hbm, hbm, vmem),
        scratch_shapes=[
            pltpu.VMEM(kv_shape, jnp.bfloat16),
            pltpu.VMEM(cq_shape, jnp.bfloat16),
            pltpu.VMEM(cs_shape, jnp.float32),
            pltpu.VMEM((depth, q_width), jnp.bfloat16),
            pltpu.VMEM((depth, META), jnp.bfloat16),
            pltpu.SemaphoreType.DMA((Q_CHUNKS,)),
            pltpu.SemaphoreType.DMA((KV_CHUNKS,)),
            pltpu.SemaphoreType.DMA((9, 3, 3)),
            pltpu.SemaphoreType.DMA((9, 3, 3)),
            pltpu.SemaphoreType.DMA((9, 4)),
            pltpu.SemaphoreType.DMA((9, 4)),
            pltpu.SemaphoreType.DMA((4,)),
        ],
        compiler_params=pltpu.CompilerParams(collective_id=0, has_side_effects=True, vmem_limit_bytes=56 * 1024 * 1024),
    )(hidden, pre, meta, cs, gain_q, gain_kv, w_dq, w_dkv)


def attend_kernel(
    cnt, cs_hbm, cq_hbm, kv_hbm, wuq_hbm, wukv_hbm, out,
    cs, cq, kv, wuq, wukv, wk, wvt, q_all, m_all, l_all, acc, sems,
):
    z, y, x, core = place()
    block = core * (RING * RING) + y * RING + x
    loads = [
        pltpu.make_async_copy(wuq_hbm.at[:, pl.ds(pl.multiple_of(block * HEADS_DEV * QK_DIM, 128), HEADS_DEV * QK_DIM)], wuq, sems.at[0]),
        pltpu.make_async_copy(cq_hbm, cq, sems.at[1]),
        pltpu.make_async_copy(cs_hbm, cs, sems.at[2]),
        pltpu.make_async_copy(wukv_hbm.at[:, pl.ds(pl.multiple_of(block * HEADS_DEV * KV_HEAD, 128), HEADS_DEV * KV_HEAD)], wukv, sems.at[3]),
        pltpu.make_async_copy(kv_hbm, kv, sems.at[4]),
    ]
    for c in loads:
        c.start()
    total = kv.shape[0] // 2
    tokens = cq.shape[0]
    n0 = total - cnt[1, META - 512].astype(jnp.int32)
    p0 = total - cnt[0, META - 512].astype(jnp.int32)
    first = z * tokens
    t = first + lax.broadcasted_iota(jnp.int32, (1, tokens), 1)
    second = t >= n0
    old_lo, old_hi = jnp.where(second, p0, 0), jnp.where(second, total, p0)
    new_lo, new_hi = jnp.where(second, total + n0, total), total + t + 1
    has0, has1 = first < n0, first + tokens > n0
    old_from = jnp.where(has0, 0, p0) // KEY_BLOCK
    old_n = (jnp.where(has1, total, p0) + KEY_BLOCK - 1) // KEY_BLOCK - old_from
    new_from = (total + jnp.where(has0, 0, n0)) // KEY_BLOCK
    new_n = (total + first + tokens) // KEY_BLOCK - new_from

    for c in loads[:3]:
        c.wait()
    q = jnp.dot(cq[...], wuq[...], preferred_element_type=jnp.float32)
    for h in range(HEADS_DEV):
        at = h * QK_DIM
        rope = turn(q[:, at + NOPE_DIM : at + QK_DIM], cs[...]).astype(jnp.bfloat16)
        q_all[h] = jnp.concatenate([q[:, at : at + NOPE_DIM].astype(jnp.bfloat16), rope, jnp.zeros_like(rope)], axis=1)
    loads[3].wait()
    for h in range(HEADS_DEV):
        at = h * KV_HEAD
        wk[:, h * 128 : h * 128 + 128] = wukv[:, at : at + NOPE_DIM]
        wvt[h * 128 : h * 128 + 128, :] = wukv[:, at + NOPE_DIM : at + KV_HEAD].T
    m_all[...] = jnp.full(m_all.shape, NEG_BIG, jnp.float32)
    l_all[...] = jnp.zeros(l_all.shape, jnp.float32)
    acc[...] = jnp.zeros(acc.shape, jnp.float32)
    loads[4].wait()
    scale = QK_DIM ** -0.5 * LOG2E
    nt = (((1,), (1,)), ((), ()))

    def body(i, carry):
        is_old = i < old_n
        row = pl.multiple_of(jnp.where(is_old, old_from + i, new_from + i - old_n) * KEY_BLOCK, KEY_BLOCK)
        lo = jnp.where(is_old, old_lo, new_lo)
        hi = jnp.where(is_old, old_hi, new_hi)
        key = row + lax.broadcasted_iota(jnp.int32, (KEY_BLOCK, tokens), 0)
        allowed = (key >= lo) & (key < hi)
        latent = kv[pl.ds(row, KEY_BLOCK), :KV_LAT]
        tail = kv[pl.ds(row, KEY_BLOCK), KV_LAT:]
        k_all = jnp.dot(latent, wk[...], preferred_element_type=jnp.float32).astype(jnp.bfloat16)
        vt = lax.dot_general(wvt[...], latent, nt, preferred_element_type=jnp.float32).astype(jnp.bfloat16)
        for h in range(HEADS_DEV):
            k = jnp.concatenate([k_all[:, h * 128 : h * 128 + 128], tail], axis=1)
            s = lax.dot_general(k, q_all[h], nt, preferred_element_type=jnp.float32)
            s = jnp.where(allowed, s, NEG_BIG)
            m_old = m_all[h]
            m_new = jnp.maximum(m_old, jnp.max(s, axis=0, keepdims=True))
            p = jnp.exp2((s - m_new) * scale)
            fade = jnp.exp2((m_old - m_new) * scale)
            m_all[h] = m_new
            l_all[h] = l_all[h] * fade + jnp.sum(p, axis=0, keepdims=True)
            acc[h] = acc[h] * fade + jnp.dot(vt[h * 128 : h * 128 + 128, :], p.astype(jnp.bfloat16), preferred_element_type=jnp.float32)
        return carry

    lax.fori_loop(0, old_n + new_n, body, 0)
    for h in range(HEADS_DEV):
        out[:, h * 128 : h * 128 + 128] = (acc[h] / l_all[h]).T.astype(jnp.bfloat16)


def attend(cnt, cs, cq, kv, w_uq, w_ukv):
    tokens, q_width = cq.shape
    hbm = pl.BlockSpec(memory_space=pl.ANY)
    return pl.pallas_call(
        attend_kernel,
        name="attend",
        out_shape=jax.ShapeDtypeStruct((tokens, HEADS_DEV * V_DIM), jnp.bfloat16),
        in_specs=[pl.BlockSpec(memory_space=pltpu.SMEM)] + [hbm] * 5,
        out_specs=pl.BlockSpec(memory_space=pltpu.VMEM),
        scratch_shapes=[
            pltpu.VMEM(cs.shape, jnp.float32),
            pltpu.VMEM(cq.shape, jnp.bfloat16),
            pltpu.VMEM(kv.shape, jnp.bfloat16),
            pltpu.VMEM((q_width, HEADS_DEV * QK_DIM), jnp.bfloat16),
            pltpu.VMEM((KV_LAT, HEADS_DEV * KV_HEAD), jnp.bfloat16),
            pltpu.VMEM((KV_LAT, HEADS_DEV * NOPE_DIM), jnp.bfloat16),
            pltpu.VMEM((HEADS_DEV * V_DIM, KV_LAT), jnp.bfloat16),
            pltpu.VMEM((HEADS_DEV, tokens, 256), jnp.bfloat16),
            pltpu.VMEM((HEADS_DEV, 1, tokens), jnp.float32),
            pltpu.VMEM((HEADS_DEV, 1, tokens), jnp.float32),
            pltpu.VMEM((HEADS_DEV, V_DIM, tokens), jnp.float32),
            pltpu.SemaphoreType.DMA((5,)),
        ],
        compiler_params=pltpu.CompilerParams(vmem_limit_bytes=56 * 1024 * 1024),
    )(cnt, cs, cq, kv, w_uq, w_ukv)


def project_kernel(o_in, wo_hbm, y_out, o_buf, w_buf, acc, other, w_sem, send_sem, recv_sem, swap_sem):
    z, y, x, core = place()
    chip = y * RING + x
    pairs = RING * RING
    depth = w_buf.shape[1]
    base = core * (pairs * depth)

    def sender(s):
        return lax.rem(y + RING - s // RING, RING) * RING + lax.rem(x + RING - lax.rem(s, RING), RING)

    def load(s):
        row = pl.multiple_of(base + sender(s) * depth, depth)
        return pltpu.make_async_copy(wo_hbm.at[pl.ds(row, depth)], w_buf.at[lax.rem(s, W_SLOTS)], w_sem.at[lax.rem(s, W_SLOTS)])

    for s in range(W_SLOTS):
        load(s).start()
    partner = index_of(z, y, x, 1 - core)
    spots = [(lax.rem(y + s // RING, RING), lax.rem(x + s % RING, RING)) for s in range(pairs)]
    greet([partner] + [index_of(z, py, px, core) for py, px in spots[1:]])
    sent = []
    for s in range(1, pairs):
        py, px = spots[s]
        row = pl.multiple_of((py * RING + px) * 2 * ROWS, 2 * ROWS)
        c = pltpu.make_async_remote_copy(
            src_ref=o_in.at[pl.ds(row, 2 * ROWS)], dst_ref=o_buf.at[chip], send_sem=send_sem.at[s], recv_sem=recv_sem.at[s],
            device_id={"sp": index_of(z, py, px, core)}, device_id_type=MESH,
        )
        c.start()
        sent.append(c)
    acc[...] = jnp.zeros(acc.shape, jnp.float32)
    cols = 1024

    def add(s, rows):
        load(s).wait()
        for n in range(acc.shape[1] // cols):
            at = slice(n * cols, n * cols + cols)
            acc[:, at] += jnp.dot(rows, w_buf[lax.rem(s, W_SLOTS), :, at], preferred_element_type=jnp.float32)

    o_buf[chip] = o_in[pl.ds(pl.multiple_of(chip * 2 * ROWS, 2 * ROWS), 2 * ROWS), :]

    def body(s, carry):
        @pl.when(s > 0)
        def _():
            got = o_buf.at[sender(s)]
            pltpu.make_async_remote_copy(src_ref=got, dst_ref=got, send_sem=send_sem.at[s], recv_sem=recv_sem.at[s], device_id={"sp": partner}, device_id_type=MESH).wait_recv()

        add(s, o_buf[sender(s)])

        @pl.when(s + W_SLOTS < pairs)
        def _():
            load(s + W_SLOTS).start()

        return carry

    lax.fori_loop(0, pairs, body, 0)
    theirs = acc.at[pl.ds(pl.multiple_of((1 - core) * ROWS, ROWS), ROWS)]
    c = pltpu.make_async_remote_copy(src_ref=theirs, dst_ref=other, send_sem=swap_sem.at[0], recv_sem=swap_sem.at[1], device_id={"sp": partner}, device_id_type=MESH)
    c.start()
    for k in sent:
        k.wait_send()
    c.wait()
    y_out[...] = (acc[pl.ds(pl.multiple_of(core * ROWS, ROWS), ROWS), :] + other[...]).astype(y_out.dtype)


def project(heads, w_o):
    width = w_o.shape[1]
    depth = heads.shape[1]
    return pl.pallas_call(
        project_kernel,
        name="project",
        out_shape=jax.ShapeDtypeStruct((ROWS, width), jnp.bfloat16),
        in_specs=[pl.BlockSpec(memory_space=pltpu.VMEM), pl.BlockSpec(memory_space=pl.ANY)],
        out_specs=pl.BlockSpec(memory_space=pltpu.VMEM),
        scratch_shapes=[
            pltpu.VMEM((RING * RING, 2 * ROWS, depth), jnp.bfloat16),
            pltpu.VMEM((W_SLOTS, depth, width), jnp.bfloat16),
            pltpu.VMEM((2 * ROWS, width), jnp.float32),
            pltpu.VMEM((ROWS, width), jnp.float32),
            pltpu.SemaphoreType.DMA((W_SLOTS,)),
            pltpu.SemaphoreType.DMA((RING * RING,)),
            pltpu.SemaphoreType.DMA((RING * RING,)),
            pltpu.SemaphoreType.DMA((2,)),
        ],
        compiler_params=pltpu.CompilerParams(collective_id=1, has_side_effects=True, vmem_limit_bytes=60 * 1024 * 1024),
    )(heads, w_o)


def solution(mesh):
    tok_spec = P(("dp", "sp"), None)
    vec_spec = P(("dp", "sp"))
    mat_spec = P(None, None)
    gain_spec = P(None)

    def device_step(hidden, seg_ids, positions, prefix_lat, prefix_seg, w_dq, gain_q, w_uq, w_dkv, gain_kv, w_ukv, w_o):
        half = ROPE_DIM // 2
        inv_freq = ROPE_BASE ** (-jnp.arange(half, dtype=jnp.float32) / half)
        angles = positions.astype(jnp.float32)[:, None] * inv_freq[None, :]
        cos_t, sin_t = jnp.cos(angles), jnp.sin(angles)
        cs = jnp.concatenate([cos_t, cos_t, -sin_t, sin_t], axis=1)
        spare = KV_WIDTH - META
        meta = jnp.pad(seg_ids.astype(jnp.bfloat16)[:, None], ((0, 0), (0, spare - 1)))
        pre = jnp.concatenate([prefix_lat, jnp.pad(prefix_seg.astype(jnp.bfloat16)[:, None], ((0, 0), (0, spare - 1)))], axis=1)
        kv, cq, cs_all, cnt = gather_latents(hidden, pre, meta, cs, gain_q[None, :], gain_kv[None, :], w_dq, w_dkv)
        heads = attend(cnt, cs_all.reshape(-1, 128), cq.reshape(-1, cq.shape[-1]), kv.reshape(-1, KV_WIDTH), w_uq, w_ukv)
        return project(heads, w_o)

    return jax.shard_map(
        device_step,
        mesh=mesh,
        in_specs=(tok_spec, vec_spec, vec_spec, tok_spec, vec_spec, mat_spec, gain_spec, mat_spec, mat_spec, gain_spec, mat_spec, mat_spec),
        out_specs=tok_spec,
        check_vma=False,
    )
```

```python
import jax
import jax.numpy as jnp
import numpy as np
from jax import lax
from jax.experimental import pallas as pl
from jax.experimental.pallas import tpu as pltpu
from jax.sharding import PartitionSpec as P

MESH = pl.DeviceIdType.MESH
KV_LAT = 512
ROPE_DIM = 64
NOPE_DIM = 128
V_DIM = 128
QK_DIM = NOPE_DIM + ROPE_DIM
KV_HEAD = NOPE_DIM + V_DIM
EPS = 1e-6
ROPE_BASE = 10000.0
NEG_BIG = -1e30
LOG2E = 1.4426950408889634
RING = 4
ROWS = 16
PLANE_TOKENS = 512
HEADS_DEV = 4
KV_WIDTH = 640
META = KV_LAT + ROPE_DIM
SPARE = KV_WIDTH - META
KEY_BLOCK = 512
W_AHEAD = 6
W_SLOTS = 4
Q_CHUNKS = 8
KV_CHUNKS = ((0, 256), (256, 256), (512, 64))


def near(array):
    return pltpu.with_memory_space_constraint(array, pltpu.VMEM)


def far(array):
    return pltpu.with_memory_space_constraint(array, pltpu.HBM)


def place():
    me = lax.axis_index("sp")
    core = lax.rem(me, 2)
    x = lax.rem(me // 2, RING)
    y = lax.rem(me // 8, RING)
    z = me // 32
    return z, y, x, core


def index_of(z, y, x, core):
    return ((z * RING + y) * RING + x) * 2 + core


def greet(peers):
    barrier = pltpu.get_barrier_semaphore()
    for peer in peers:
        pl.semaphore_signal(barrier, inc=1, device_id={"sp": peer}, device_id_type=MESH)
    pl.semaphore_wait(barrier, len(peers))


class Stream:
    def __init__(self, slot, ref, axes, order, lanes, sems):
        self.slot, self.ref, self.axes, self.order, self.lanes = slot, ref, axes, order, lanes
        self.send_sem, self.recv_sem, self.swap_send, self.swap_recv = sems
        z, y, x, self.core = place()
        self.at = (z, y, x)
        self.sent = []

    def view(self, full, core, moved=None, half=None):
        index = []
        for axis in self.axes:
            if axis in full:
                both = half is None or axis != full[0]
                index.append(pl.ds(0, RING) if both else pl.ds(half * (RING // 2), RING // 2))
            elif moved is not None and moved[0] == axis:
                index.append(moved[1])
            else:
                index.append(self.at[axis])
        return self.ref.at[tuple(index) + (core, slice(None), self.lanes)]

    def back(self, axis, off):
        return lax.rem(self.at[axis] + RING - off, RING)

    def ahead(self, axis, off):
        to = list(self.at)
        to[axis] = lax.rem(self.at[axis] + off, RING)
        return index_of(*to, self.core)

    def copy(self, part, phase, slot, device):
        return pltpu.make_async_remote_copy(
            src_ref=part, dst_ref=part, send_sem=self.send_sem.at[self.slot, phase, slot], recv_sem=self.recv_sem.at[self.slot, phase, slot],
            device_id={"sp": device}, device_id_type=MESH,
        )

    def push(self, part, phase, slot, device):
        c = self.copy(part, phase, slot, device)
        c.start()
        self.sent.append(c)

    def swap_copy(self, off, core):
        part = self.view(self.order[:-1], core, (self.order[-1], self.back(self.order[-1], off)))
        return pltpu.make_async_remote_copy(
            src_ref=part, dst_ref=part, send_sem=self.swap_send.at[self.slot, off], recv_sem=self.swap_recv.at[self.slot, off],
            device_id={"sp": index_of(*self.at, 1 - self.core)}, device_id_type=MESH,
        )

    def swap(self, off):
        c = self.swap_copy(off, self.core)
        c.start()
        self.sent.append(c)

    def send(self, phase):
        last = phase == len(self.order) - 1
        mine = self.view(self.order[:phase], self.core)
        for off in (1, 3) if last else (1, 3, 2):
            self.push(mine, phase, off - 1, self.ahead(self.order[phase], off))
        if last:
            self.swap(0)

    def wait(self, phase, off):
        axis = self.order[phase]
        got = self.view(self.order[:phase], self.core, (axis, self.back(axis, off)))
        self.copy(got, phase, off - 1, self.ahead(axis, 1)).wait_recv()

    def step(self, phase):
        for off in (1, 3, 2):
            self.wait(phase - 1, off)
        self.send(phase)

    def relay(self):
        last = len(self.order) - 1
        axis = self.order[last]
        for off, half, slot in ((1, 0, 1), (3, 1, 3)):
            self.wait(last, off)
            part = self.view(self.order[:last], self.core, (axis, self.back(axis, off)), half)
            self.push(part, last, slot, self.ahead(axis, off))
            self.swap(off)

    def finish(self):
        last = len(self.order) - 1
        axis = self.order[last]
        for half, slot in ((0, 1), (1, 3)):
            part = self.view(self.order[:last], self.core, (axis, self.back(axis, 2)), half)
            self.copy(part, last, slot, self.ahead(axis, 1)).wait_recv()
        self.swap(2)

    def done(self):
        for off in (0, 1, 3, 2):
            self.swap_copy(off, 1 - self.core).wait_recv()
        for c in self.sent:
            c.wait_send()


def rms_norm(values, gain):
    inv_rms = lax.rsqrt(jnp.mean(values * values, axis=-1, keepdims=True) + EPS)
    return values * inv_rms * gain


def turn(values, cos_sin):
    half = ROPE_DIM // 2
    swapped = jnp.concatenate([values[:, half:], values[:, :half]], axis=1)
    return values * cos_sin[:, :ROPE_DIM] + swapped * cos_sin[:, ROPE_DIM:]


def rows_of(scalars, width):
    row = lax.broadcasted_iota(jnp.int32, (ROWS, width), 0)
    values = jnp.zeros((ROWS, width), jnp.int32)
    for r in range(ROWS):
        values = jnp.where(row == r, scalars[r], values)
    return values


def prompt_flags(seg):
    values = rows_of(seg, SPARE)
    lane = lax.broadcasted_iota(jnp.int32, values.shape, 1)
    return ((lane < 2) & (lane == values)).astype(jnp.float32).astype(jnp.bfloat16)


def gather_kernel(
    pos_hbm, seg_hbm, old_seg_hbm, hid_hbm, old_lat_hbm, freq_hbm, gain_q_hbm, gain_kv_hbm, wdq_hbm, wdkv_hbm,
    kv_buf, cq_buf, cs_buf,
    pos, seg, old_seg, hid, old_lat, freq, gain_q, gain_kv, small_sem, wq_buf, wkv_buf, wq_sem, wkv_sem, send_sem, recv_sem, swap_send, swap_recv,
):
    z, y, x, core = place()
    depth = hid_hbm.shape[1]
    q_step = depth // Q_CHUNKS
    kv_loads = [pltpu.make_async_copy(wdkv_hbm.at[pl.ds(at, n)], wkv_buf.at[pl.ds(at, n)], wkv_sem.at[k]) for k, (at, n) in enumerate(KV_CHUNKS)]
    q_loads = [pltpu.make_async_copy(wdq_hbm.at[pl.ds(k * q_step, q_step)], wq_buf.at[pl.ds(k * q_step, q_step)], wq_sem.at[k]) for k in range(Q_CHUNKS)]
    pairs = (
        (pos_hbm, pos), (old_seg_hbm, old_seg), (old_lat_hbm, old_lat), (freq_hbm, freq),
        (seg_hbm, seg), (hid_hbm, hid), (gain_kv_hbm, gain_kv), (gain_q_hbm, gain_q),
    )
    small = [pltpu.make_async_copy(src, dst, small_sem.at[k]) for k, (src, dst) in enumerate(pairs)]
    for c in small + kv_loads + q_loads:
        c.start()
    for c in small:
        c.wait()

    kv_buf[0, z, y, x, core] = jnp.concatenate([old_lat[...], prompt_flags(old_seg)], axis=1)
    angles = rows_of(pos, 128).astype(jnp.float32) * freq[...]
    lane = lax.broadcasted_iota(jnp.int32, angles.shape, 1)
    sines = jnp.sin(angles)
    cs = jnp.where(lane < ROPE_DIM, jnp.cos(angles), jnp.where(lane < ROPE_DIM + ROPE_DIM // 2, -sines, sines))
    cs_buf[y, x, core] = cs

    peers = [index_of(z, y, x, 1 - core)]
    for off in (1, 2, 3):
        peers.append(index_of(lax.rem(z + off, RING), y, x, core))
        peers.append(index_of(z, lax.rem(y + off, RING), x, core))
        peers.append(index_of(z, y, lax.rem(x + off, RING), core))
    greet(peers)

    sems = (send_sem, recv_sem, swap_send, swap_recv)
    lanes = (pl.ds(0, 256), pl.ds(256, 256), pl.ds(512, 128))
    space = (0, 1, 2)
    plane = (1, 2)
    to_z, to_y, to_x = (2, 1, 0), (0, 2, 1), (1, 0, 2)
    old = [Stream(i, kv_buf.at[0], space, (to_z, to_x, to_y)[i], lanes[i], sems) for i in range(3)]
    new = [Stream(3 + i, kv_buf.at[1], space, (to_z, to_y, to_x)[i], lanes[i], sems) for i in range(3)]
    half = cq_buf.shape[-1] // 2
    lat = [Stream(6, cq_buf, plane, (2, 1), pl.ds(0, half), sems), Stream(7, cq_buf, plane, (1, 2), pl.ds(half, half), sems)]
    turns = [Stream(8, cs_buf, plane, (2, 1), pl.ds(0, 128), sems)]
    for s in old + turns:
        s.send(0)

    nt = (((1,), (1,)), ((), ()))
    down = []
    for k, (at, n) in enumerate(KV_CHUNKS):
        kv_loads[k].wait()
        down.append(lax.dot_general(hid[...], wkv_buf[at : at + n, :], nt, preferred_element_type=jnp.float32))
    kv_lat = rms_norm(jnp.concatenate(down[:-1], axis=1), gain_kv[...].astype(jnp.float32).reshape(1, -1)).astype(jnp.bfloat16)
    key_rope = turn(down[-1], cs).astype(jnp.bfloat16)
    kv_buf[1, z, y, x, core] = jnp.concatenate([kv_lat, key_rope, prompt_flags(seg)], axis=1)
    for s in old + turns:
        s.step(1)
    for s in new:
        s.send(0)

    q_lat = jnp.zeros((ROWS, wq_buf.shape[1]), jnp.float32)
    for k in range(Q_CHUNKS):
        q_loads[k].wait()
        part = pl.ds(k * q_step, q_step)
        q_lat = q_lat + jnp.dot(hid[:, part], wq_buf[part, :], preferred_element_type=jnp.float32)
        if k == 4:
            for s in old:
                s.step(2)
            for s in new:
                s.step(1)
    cq_buf[y, x, core] = rms_norm(q_lat, gain_q[...].astype(jnp.float32).reshape(1, -1)).astype(jnp.bfloat16)
    for s in lat:
        s.send(0)
    for s in turns + old:
        s.relay()
    for s in new:
        s.step(2)
    for s in lat:
        s.step(1)
    for s in turns + old:
        s.finish()
    for s in new + lat:
        s.relay()
    for s in new + lat:
        s.finish()
    for s in turns + old + new + lat:
        s.done()


def gather_latents(positions, seg_ids, prefix_seg, hidden, prefix_lat, gain_q, gain_kv, w_dq, w_dkv_t):
    depth, q_width = w_dq.shape
    half = ROPE_DIM // 2
    freq = np.float32(ROPE_BASE) ** (-np.arange(half, dtype=np.float32) / np.float32(half))
    freq = np.tile(freq, 128 // half)[None, :].astype(np.float32)
    vmem = pl.BlockSpec(memory_space=pltpu.VMEM)
    hbm = pl.BlockSpec(memory_space=pl.ANY)
    return pl.pallas_call(
        gather_kernel,
        name="gather_latents",
        out_shape=(
            pltpu.VMEM((2, RING, RING, RING, 2, ROWS, KV_WIDTH), jnp.bfloat16),
            pltpu.VMEM((RING, RING, 2, ROWS, q_width), jnp.bfloat16),
            pltpu.VMEM((RING, RING, 2, ROWS, 128), jnp.float32),
        ),
        in_specs=[hbm] * 10,
        out_specs=(vmem,) * 3,
        scratch_shapes=[
            pltpu.SMEM((ROWS,), jnp.int32),
            pltpu.SMEM((ROWS,), jnp.int32),
            pltpu.SMEM((ROWS,), jnp.int32),
            pltpu.VMEM(hidden.shape, jnp.bfloat16),
            pltpu.VMEM(prefix_lat.shape, jnp.bfloat16),
            pltpu.VMEM(freq.shape, jnp.float32),
            pltpu.VMEM(gain_q.shape, jnp.bfloat16),
            pltpu.VMEM(gain_kv.shape, jnp.bfloat16),
            pltpu.SemaphoreType.DMA((8,)),
            pltpu.VMEM((depth, q_width), jnp.bfloat16),
            pltpu.VMEM((META, depth), jnp.bfloat16),
            pltpu.SemaphoreType.DMA((Q_CHUNKS,)),
            pltpu.SemaphoreType.DMA((len(KV_CHUNKS),)),
            pltpu.SemaphoreType.DMA((9, 3, 4)),
            pltpu.SemaphoreType.DMA((9, 3, 4)),
            pltpu.SemaphoreType.DMA((9, 4)),
            pltpu.SemaphoreType.DMA((9, 4)),
        ],
        compiler_params=pltpu.CompilerParams(collective_id=0, has_side_effects=True, vmem_limit_bytes=24 * 1024 * 1024),
    )(*map(far, (positions, seg_ids, prefix_seg, hidden, prefix_lat, jnp.asarray(freq), gain_q, gain_kv, w_dq, w_dkv_t)))


def sender(z, y, x, s):
    return lax.rem(y + RING - s // RING, RING) * RING + lax.rem(x + RING - lax.rem(s, RING), RING)


def attend_kernel(
    cs, cq, kv, wuq_hbm, wukv_hbm, wo_hbm, out, w_ahead,
    wuq, wukv, wk, wvt, q_all, m_all, l_all, acc, sems, w_sem,
):
    z, y, x, core = place()
    block = core * (RING * RING) + y * RING + x
    loads = [
        pltpu.make_async_copy(wuq_hbm.at[:, pl.ds(pl.multiple_of(block * HEADS_DEV * QK_DIM, 128), HEADS_DEV * QK_DIM)], wuq, sems.at[0]),
        pltpu.make_async_copy(wukv_hbm.at[:, pl.ds(pl.multiple_of(block * HEADS_DEV * KV_HEAD, 128), HEADS_DEV * KV_HEAD)], wukv, sems.at[1]),
    ]
    depth = w_ahead.shape[1]
    for s in range(W_AHEAD):
        row = pl.multiple_of((core * (RING * RING) + sender(z, y, x, s)) * depth, depth)
        loads.append(pltpu.make_async_copy(wo_hbm.at[pl.ds(row, depth)], w_ahead.at[s], w_sem.at[s]))
    for c in loads:
        c.start()
    total = kv.shape[0] // 2
    tokens = cq.shape[0]

    def first_rows(sec):
        flags = kv[pl.ds(sec * total, total), pl.ds(KV_LAT, 128)].astype(jnp.float32)
        lane = lax.broadcasted_iota(jnp.int32, (1, 128), 1)
        return jnp.sum(jnp.where(lane == ROPE_DIM, jnp.sum(flags, axis=0, keepdims=True), 0.0)).astype(jnp.int32)

    p0, n0 = first_rows(0), first_rows(1)
    first = z * tokens
    has0, has1 = first < n0, first + tokens > n0
    old_from = jnp.where(has0, 0, p0) // KEY_BLOCK
    old_n = (jnp.where(has1, total, p0) + KEY_BLOCK - 1) // KEY_BLOCK - old_from
    new_from = (total + jnp.where(has0, 0, n0)) // KEY_BLOCK
    new_n = (total + first) // KEY_BLOCK - new_from

    token = first + lax.broadcasted_iota(jnp.int32, (tokens, SPARE), 0)
    lane = lax.broadcasted_iota(jnp.int32, (tokens, SPARE), 1)
    other = jnp.where(token >= n0, 0, 1)
    gate = jnp.where(lane == other, NEG_BIG, 0.0).astype(jnp.bfloat16)

    loads[0].wait()
    q = jnp.dot(cq[...], wuq[...], preferred_element_type=jnp.float32)
    for h in range(HEADS_DEV):
        at = h * QK_DIM
        rope = turn(q[:, at + NOPE_DIM : at + QK_DIM], cs[...]).astype(jnp.bfloat16)
        q_all[h] = jnp.concatenate([q[:, at : at + NOPE_DIM].astype(jnp.bfloat16), rope, gate], axis=1)
    loads[1].wait()
    for h in range(HEADS_DEV):
        at = h * KV_HEAD
        wk[:, h * 128 : h * 128 + 128] = wukv[:, at : at + NOPE_DIM]
        wvt[h * 128 : h * 128 + 128, :] = wukv[:, at + NOPE_DIM : at + KV_HEAD].T
    scale = QK_DIM ** -0.5 * LOG2E
    nt = (((1,), (1,)), ((), ()))

    def block_of(row, size, start):
        latent = kv[pl.ds(row, size), :KV_LAT]
        tail = kv[pl.ds(row, size), KV_LAT:]
        k_all = jnp.dot(latent, wk[...], preferred_element_type=jnp.float32).astype(jnp.bfloat16)
        vt = lax.dot_general(wvt[...], latent, nt, preferred_element_type=jnp.float32).astype(jnp.bfloat16)

        def score(h):
            k = jnp.concatenate([k_all[:, h * 128 : h * 128 + 128], tail], axis=1)
            return lax.dot_general(k, q_all[h], nt, preferred_element_type=jnp.float32)

        ahead = score(0)
        for h in range(HEADS_DEV):
            s = ahead
            if h + 1 < HEADS_DEV:
                ahead = score(h + 1)
            v = vt[h * 128 : h * 128 + 128, :]
            if start:
                causal = lax.broadcasted_iota(jnp.int32, s.shape, 0) <= lax.broadcasted_iota(jnp.int32, s.shape, 1)
                s = jnp.where(causal, s, NEG_BIG)
                m_new = jnp.max(s, axis=0, keepdims=True)
                p = jnp.exp2((s - m_new) * scale)
                l_all[h] = jnp.sum(p, axis=0, keepdims=True)
                acc[h] = jnp.dot(v, p.astype(jnp.bfloat16), preferred_element_type=jnp.float32)
            else:
                m_old = m_all[h]
                m_new = jnp.maximum(m_old, jnp.max(s, axis=0, keepdims=True))
                p = jnp.exp2((s - m_new) * scale)
                fade = jnp.exp2((m_old - m_new) * scale)
                l_all[h] = l_all[h] * fade + jnp.sum(p, axis=0, keepdims=True)
                acc[h] = acc[h] * fade + jnp.dot(v, p.astype(jnp.bfloat16), preferred_element_type=jnp.float32)
            m_all[h] = m_new

    block_of(pl.multiple_of(total + first, tokens), tokens, True)

    def body(i, carry):
        row = jnp.where(i < old_n, old_from + i, new_from + i - old_n) * KEY_BLOCK
        block_of(pl.multiple_of(row, KEY_BLOCK), KEY_BLOCK, False)
        return carry

    lax.fori_loop(0, old_n + new_n, body, 0)
    for h in range(HEADS_DEV):
        out[:, h * 128 : h * 128 + 128] = (acc[h] / l_all[h]).T.astype(jnp.bfloat16)
    for c in loads[2:]:
        c.wait()


def attend(cs, cq, kv, w_uq, w_ukv, w_o):
    tokens, q_width = cq.shape
    hbm = pl.BlockSpec(memory_space=pl.ANY)
    vmem = pl.BlockSpec(memory_space=pltpu.VMEM)
    return pl.pallas_call(
        attend_kernel,
        name="attend",
        out_shape=(
            pltpu.VMEM((tokens, HEADS_DEV * V_DIM), jnp.bfloat16),
            pltpu.VMEM((W_AHEAD, HEADS_DEV * V_DIM, w_o.shape[1]), jnp.bfloat16),
        ),
        in_specs=[vmem] * 3 + [hbm] * 3,
        out_specs=(vmem, vmem),
        scratch_shapes=[
            pltpu.VMEM((q_width, HEADS_DEV * QK_DIM), jnp.bfloat16),
            pltpu.VMEM((KV_LAT, HEADS_DEV * KV_HEAD), jnp.bfloat16),
            pltpu.VMEM((KV_LAT, HEADS_DEV * NOPE_DIM), jnp.bfloat16),
            pltpu.VMEM((HEADS_DEV * V_DIM, KV_LAT), jnp.bfloat16),
            pltpu.VMEM((HEADS_DEV, tokens, 256), jnp.bfloat16),
            pltpu.VMEM((HEADS_DEV, 1, tokens), jnp.float32),
            pltpu.VMEM((HEADS_DEV, 1, tokens), jnp.float32),
            pltpu.VMEM((HEADS_DEV, V_DIM, tokens), jnp.float32),
            pltpu.SemaphoreType.DMA((2,)),
            pltpu.SemaphoreType.DMA((W_AHEAD,)),
        ],
        compiler_params=pltpu.CompilerParams(vmem_limit_bytes=14 * 1024 * 1024),
    )(cs, cq, kv, w_uq, w_ukv, w_o)


def project_kernel(o_in, w_ahead, wo_hbm, y_out, o_buf, w_buf, acc, other, w_sem, send_sem, recv_sem, swap_sem):
    z, y, x, core = place()
    chip = y * RING + x
    pairs = RING * RING
    depth = w_buf.shape[1]
    base = core * (pairs * depth)

    def load(s):
        row = pl.multiple_of(base + sender(z, y, x, s) * depth, depth)
        return pltpu.make_async_copy(wo_hbm.at[pl.ds(row, depth)], w_buf.at[lax.rem(s - W_AHEAD, W_SLOTS)], w_sem.at[lax.rem(s - W_AHEAD, W_SLOTS)])

    for s in range(W_SLOTS):
        load(W_AHEAD + s).start()
    partner = index_of(z, y, x, 1 - core)
    spots = [(lax.rem(y + s // RING, RING), lax.rem(x + s % RING, RING)) for s in range(pairs)]
    greet([partner] + [index_of(z, py, px, core) for py, px in spots[1:]])
    sent = []
    for s in range(1, pairs):
        py, px = spots[s]
        row = pl.multiple_of((py * RING + px) * 2 * ROWS, 2 * ROWS)
        c = pltpu.make_async_remote_copy(
            src_ref=o_in.at[pl.ds(row, 2 * ROWS)], dst_ref=o_buf.at[chip], send_sem=send_sem.at[s], recv_sem=recv_sem.at[s],
            device_id={"sp": index_of(z, py, px, core)}, device_id_type=MESH,
        )
        c.start()
        sent.append(c)
    acc[...] = jnp.zeros(acc.shape, jnp.float32)
    cols = 1024

    def add(s, w):
        rows = o_buf[sender(z, y, x, s)]
        for n in range(acc.shape[1] // cols):
            at = slice(n * cols, n * cols + cols)
            acc[:, at] += jnp.dot(rows, w[:, at], preferred_element_type=jnp.float32)

    def arrive(s):
        got = o_buf.at[sender(z, y, x, s)]
        pltpu.make_async_remote_copy(src_ref=got, dst_ref=got, send_sem=send_sem.at[s], recv_sem=recv_sem.at[s], device_id={"sp": partner}, device_id_type=MESH).wait_recv()

    o_buf[chip] = o_in[pl.ds(pl.multiple_of(chip * 2 * ROWS, 2 * ROWS), 2 * ROWS), :]

    def held(s, carry):
        @pl.when(s > 0)
        def _():
            arrive(s)

        add(s, w_ahead.at[s])
        return carry

    def streamed(s, carry):
        arrive(s)
        load(s).wait()
        add(s, w_buf.at[lax.rem(s - W_AHEAD, W_SLOTS)])

        @pl.when(s + W_SLOTS < pairs)
        def _():
            load(s + W_SLOTS).start()

        return carry

    lax.fori_loop(0, W_AHEAD, held, 0)
    lax.fori_loop(W_AHEAD, pairs, streamed, 0)
    theirs = acc.at[pl.ds(pl.multiple_of((1 - core) * ROWS, ROWS), ROWS)]
    c = pltpu.make_async_remote_copy(src_ref=theirs, dst_ref=other, send_sem=swap_sem.at[0], recv_sem=swap_sem.at[1], device_id={"sp": partner}, device_id_type=MESH)
    c.start()
    for k in sent:
        k.wait_send()
    c.wait()
    y_out[...] = (acc[pl.ds(pl.multiple_of(core * ROWS, ROWS), ROWS), :] + other[...]).astype(y_out.dtype)


def project(heads, w_ahead, w_o):
    width = w_o.shape[1]
    depth = heads.shape[1]
    return pl.pallas_call(
        project_kernel,
        name="project",
        out_shape=jax.ShapeDtypeStruct((ROWS, width), jnp.bfloat16),
        in_specs=[pl.BlockSpec(memory_space=pltpu.VMEM)] * 2 + [pl.BlockSpec(memory_space=pl.ANY)],
        out_specs=pl.BlockSpec(memory_space=pltpu.VMEM),
        scratch_shapes=[
            pltpu.VMEM((RING * RING, 2 * ROWS, depth), jnp.bfloat16),
            pltpu.VMEM((W_SLOTS, depth, width), jnp.bfloat16),
            pltpu.VMEM((2 * ROWS, width), jnp.float32),
            pltpu.VMEM((ROWS, width), jnp.float32),
            pltpu.SemaphoreType.DMA((W_SLOTS,)),
            pltpu.SemaphoreType.DMA((RING * RING,)),
            pltpu.SemaphoreType.DMA((RING * RING,)),
            pltpu.SemaphoreType.DMA((2,)),
        ],
        compiler_params=pltpu.CompilerParams(collective_id=1, has_side_effects=True, vmem_limit_bytes=24 * 1024 * 1024),
    )(heads, w_ahead, w_o)


def solution(mesh):
    tok_spec = P(("dp", "sp"), None)
    vec_spec = P(("dp", "sp"))
    mat_spec = P(None, None)
    gain_spec = P(None)

    def device_step(hidden, seg_ids, positions, prefix_lat, prefix_seg, w_dq, gain_q, w_uq, w_dkv, gain_kv, w_ukv, w_o):
        kv, cq, cs = gather_latents(positions, seg_ids, prefix_seg, hidden, prefix_lat, gain_q, gain_kv, w_dq, w_dkv.T)
        heads, w_ahead = attend(near(cs.reshape(-1, 128)), near(cq.reshape(-1, cq.shape[-1])), near(kv.reshape(-1, KV_WIDTH)), w_uq, w_ukv, w_o)
        return project(near(heads), near(w_ahead), w_o)

    return jax.shard_map(
        device_step,
        mesh=mesh,
        in_specs=(tok_spec, vec_spec, vec_spec, tok_spec, vec_spec, mat_spec, gain_spec, mat_spec, mat_spec, gain_spec, mat_spec, mat_spec),
        out_specs=tok_spec,
        check_vma=False,
    )
```

```python
import jax
import jax.numpy as jnp
import numpy as np
from jax import lax
from jax.experimental import pallas as pl
from jax.experimental.pallas import tpu as pltpu
from jax.sharding import PartitionSpec as P

MESH = pl.DeviceIdType.MESH
KV_LAT = 512
ROPE_DIM = 64
NOPE_DIM = 128
V_DIM = 128
QK_DIM = NOPE_DIM + ROPE_DIM
KV_HEAD = NOPE_DIM + V_DIM
EPS = 1e-6
ROPE_BASE = 10000.0
NEG_BIG = -1e30
LOG2E = 1.4426950408889634
RING = 4
ROWS = 16
PLANE_TOKENS = 512
HEADS_DEV = 4
KV_WIDTH = 640
META = KV_LAT + ROPE_DIM
SPARE = KV_WIDTH - META
KEY_BLOCK = 512
W_AHEAD = 6
W_SLOTS = 8
Q_FLIGHT = 4
Q_SLOTS = 5
VMEM_LIMIT = 13 * 1024 * 1024 + 256 * 1024
Q_CHUNKS = 16
KV_CHUNKS = ((0, 256), (256, 256), (512, 64))


def near(array):
    return pltpu.with_memory_space_constraint(array, pltpu.VMEM)


def far(array):
    return pltpu.with_memory_space_constraint(array, pltpu.HBM)


def place():
    me = lax.axis_index("sp")
    core = lax.rem(me, 2)
    x = lax.rem(me // 2, RING)
    y = lax.rem(me // 8, RING)
    z = me // 32
    return z, y, x, core


def index_of(z, y, x, core):
    return ((z * RING + y) * RING + x) * 2 + core


def greet(peers):
    barrier = pltpu.get_barrier_semaphore()
    for peer in peers:
        pl.semaphore_signal(barrier, inc=1, device_id={"sp": peer}, device_id_type=MESH)
    return lambda: pl.semaphore_wait(barrier, len(peers))


class Stream:
    def __init__(self, slot, ref, axes, order, lanes, sems):
        self.slot, self.ref, self.axes, self.order, self.lanes = slot, ref, axes, order, lanes
        self.send_sem, self.recv_sem, self.swap_send, self.swap_recv = sems
        z, y, x, self.core = place()
        self.at = (z, y, x)
        self.sent = []

    def view(self, full, core, moved=None, half=None):
        index = []
        for axis in self.axes:
            if axis in full:
                both = half is None or axis != full[0]
                index.append(pl.ds(0, RING) if both else pl.ds(half * (RING // 2), RING // 2))
            elif moved is not None and moved[0] == axis:
                index.append(moved[1])
            else:
                index.append(self.at[axis])
        return self.ref.at[tuple(index) + (core, slice(None), self.lanes)]

    def back(self, axis, off):
        return lax.rem(self.at[axis] + RING - off, RING)

    def ahead(self, axis, off):
        to = list(self.at)
        to[axis] = lax.rem(self.at[axis] + off, RING)
        return index_of(*to, self.core)

    def copy(self, part, phase, slot, device):
        return pltpu.make_async_remote_copy(
            src_ref=part, dst_ref=part, send_sem=self.send_sem.at[self.slot, phase, slot], recv_sem=self.recv_sem.at[self.slot, phase, slot],
            device_id={"sp": device}, device_id_type=MESH,
        )

    def push(self, part, phase, slot, device):
        c = self.copy(part, phase, slot, device)
        c.start()
        self.sent.append(c)

    def swap_copy(self, off, core):
        part = self.view(self.order[:-1], core, (self.order[-1], self.back(self.order[-1], off)))
        return pltpu.make_async_remote_copy(
            src_ref=part, dst_ref=part, send_sem=self.swap_send.at[self.slot, off], recv_sem=self.swap_recv.at[self.slot, off],
            device_id={"sp": index_of(*self.at, 1 - self.core)}, device_id_type=MESH,
        )

    def swap(self, off):
        c = self.swap_copy(off, self.core)
        c.start()
        self.sent.append(c)

    def send(self, phase):
        last = phase == len(self.order) - 1
        mine = self.view(self.order[:phase], self.core)
        for off in (1, 3) if last else (1, 3, 2):
            self.push(mine, phase, off - 1, self.ahead(self.order[phase], off))
        if last:
            self.swap(0)

    def wait(self, phase, off):
        axis = self.order[phase]
        got = self.view(self.order[:phase], self.core, (axis, self.back(axis, off)))
        self.copy(got, phase, off - 1, self.ahead(axis, 1)).wait_recv()

    def step(self, phase):
        for off in (1, 3, 2):
            self.wait(phase - 1, off)
        self.send(phase)

    def relay(self):
        last = len(self.order) - 1
        axis = self.order[last]
        for off, half, slot in ((1, 0, 1), (3, 1, 3)):
            self.wait(last, off)
            part = self.view(self.order[:last], self.core, (axis, self.back(axis, off)), half)
            self.push(part, last, slot, self.ahead(axis, off))
            self.swap(off)

    def finish(self):
        last = len(self.order) - 1
        axis = self.order[last]
        for half, slot in ((0, 1), (1, 3)):
            part = self.view(self.order[:last], self.core, (axis, self.back(axis, 2)), half)
            self.copy(part, last, slot, self.ahead(axis, 1)).wait_recv()
        self.swap(2)

    def done(self):
        for off in (0, 1, 3, 2):
            self.swap_copy(off, 1 - self.core).wait_recv()
        for c in self.sent:
            c.wait_send()


def rms_norm(values, gain):
    inv_rms = lax.rsqrt(jnp.mean(values * values, axis=-1, keepdims=True) + EPS)
    return values * inv_rms * gain


def turn(values, cos_sin):
    half = ROPE_DIM // 2
    swapped = jnp.concatenate([values[:, half:], values[:, :half]], axis=1)
    return values * cos_sin[:, :ROPE_DIM] + swapped * cos_sin[:, ROPE_DIM:]


def rows_of(scalars, width):
    row = lax.broadcasted_iota(jnp.int32, (ROWS, width), 0)
    values = jnp.zeros((ROWS, width), jnp.int32)
    for r in range(ROWS):
        values = jnp.where(row == r, scalars[r], values)
    return values


def prompt_flags(seg):
    values = rows_of(seg, SPARE)
    lane = lax.broadcasted_iota(jnp.int32, values.shape, 1)
    return ((lane < 2) & (lane == values)).astype(jnp.float32).astype(jnp.bfloat16)


def gather_kernel(
    pos_hbm, seg_hbm, old_seg_hbm, hid_hbm, old_lat_hbm, freq_hbm, gain_q_hbm, gain_kv_hbm, wdq_hbm, wdkv_hbm, wuq_hbm, wukv_hbm,
    kv_buf, cq_buf, cs_buf, wuq, wukv,
    pos, seg, old_seg, hid, old_lat, freq, gain_q, gain_kv, small_sem, head_sem, wq_buf, wkv_buf, wq_sem, wkv_sem, send_sem, recv_sem, swap_send, swap_recv,
):
    z, y, x, core = place()
    depth = hid_hbm.shape[1]
    q_step = depth // Q_CHUNKS
    kv_loads = [pltpu.make_async_copy(wdkv_hbm.at[pl.ds(at, n)], wkv_buf.at[pl.ds(at, n)], wkv_sem.at[k]) for k, (at, n) in enumerate(KV_CHUNKS)]
    q_loads = [pltpu.make_async_copy(wdq_hbm.at[pl.ds(k * q_step, q_step)], wq_buf.at[k % Q_SLOTS], wq_sem.at[k]) for k in range(Q_CHUNKS)]
    pairs = (
        (pos_hbm, pos), (old_seg_hbm, old_seg), (old_lat_hbm, old_lat), (freq_hbm, freq),
        (seg_hbm, seg), (hid_hbm, hid), (gain_kv_hbm, gain_kv), (gain_q_hbm, gain_q),
    )
    block = core * (RING * RING) + y * RING + x
    heads = [
        pltpu.make_async_copy(src.at[:, pl.ds(pl.multiple_of(block * dst.shape[1], 128), dst.shape[1])], dst, head_sem.at[k])
        for k, (src, dst) in enumerate(((wuq_hbm, wuq), (wukv_hbm, wukv)))
    ]
    small = [pltpu.make_async_copy(src, dst, small_sem.at[k]) for k, (src, dst) in enumerate(pairs)]
    for c in small + kv_loads:
        c.start()
    peers = [index_of(z, y, x, 1 - core)]
    for off in (1, 2, 3):
        peers.append(index_of(lax.rem(z + off, RING), y, x, core))
        peers.append(index_of(z, lax.rem(y + off, RING), x, core))
        peers.append(index_of(z, y, lax.rem(x + off, RING), core))
    all_here = greet(peers)
    for c in small:
        c.wait()
    for c in q_loads[:Q_FLIGHT]:
        c.start()

    kv_buf[0, z, y, x, core] = jnp.concatenate([old_lat[...], prompt_flags(old_seg)], axis=1)
    angles = rows_of(pos, 128).astype(jnp.float32) * freq[...]
    lane = lax.broadcasted_iota(jnp.int32, angles.shape, 1)
    sines = jnp.sin(angles)
    cs = jnp.where(lane < ROPE_DIM, jnp.cos(angles), jnp.where(lane < ROPE_DIM + ROPE_DIM // 2, -sines, sines))
    cs_buf[y, x, core] = cs

    all_here()

    sems = (send_sem, recv_sem, swap_send, swap_recv)
    lanes = (pl.ds(0, 256), pl.ds(256, 256), pl.ds(512, 128))
    space = (0, 1, 2)
    plane = (1, 2)
    to_z, to_y, to_x = (2, 1, 0), (0, 2, 1), (1, 0, 2)
    old = [Stream(i, kv_buf.at[0], space, (to_z, to_x, to_y)[i], lanes[i], sems) for i in range(3)]
    new = [Stream(3 + i, kv_buf.at[1], space, (to_z, to_y, to_x)[i], lanes[i], sems) for i in range(3)]
    half = cq_buf.shape[-1] // 2
    lat = [Stream(6, cq_buf, plane, (2, 1), pl.ds(0, half), sems), Stream(7, cq_buf, plane, (1, 2), pl.ds(half, half), sems)]
    turns = [Stream(8, cs_buf, plane, (2, 1), pl.ds(0, 128), sems)]
    for s in old + turns:
        s.send(0)

    nt = (((1,), (1,)), ((), ()))
    down = []
    for k, (at, n) in enumerate(KV_CHUNKS):
        kv_loads[k].wait()
        down.append(lax.dot_general(hid[...], wkv_buf[at : at + n, :], nt, preferred_element_type=jnp.float32))
    kv_lat = rms_norm(jnp.concatenate(down[:-1], axis=1), gain_kv[...].astype(jnp.float32).reshape(1, -1)).astype(jnp.bfloat16)
    key_rope = turn(down[-1], cs).astype(jnp.bfloat16)
    kv_buf[1, z, y, x, core] = jnp.concatenate([kv_lat, key_rope, prompt_flags(seg)], axis=1)
    for s in new:
        s.send(0)

    q_lat = jnp.zeros((ROWS, wq_buf.shape[2]), jnp.float32)
    for k in range(Q_CHUNKS):
        q_loads[k].wait()
        if k + Q_FLIGHT < Q_CHUNKS:
            q_loads[k + Q_FLIGHT].start()
        elif k + Q_FLIGHT == Q_CHUNKS:
            for c in heads:
                c.start()
        part = pl.ds(k * q_step, q_step)
        q_lat = q_lat + jnp.dot(hid[:, part], wq_buf[k % Q_SLOTS], preferred_element_type=jnp.float32)
        if k == 5:
            for s in old + turns:
                s.step(1)
        if k == 11:
            for s in new:
                s.step(1)
    cq_buf[y, x, core] = rms_norm(q_lat, gain_q[...].astype(jnp.float32).reshape(1, -1)).astype(jnp.bfloat16)
    for s in lat:
        s.send(0)
    for s in old:
        s.step(2)
    for s in turns:
        s.relay()
    for s in new:
        s.step(2)
    for s in lat:
        s.step(1)
    for s in turns:
        s.finish()
    for s in old + new + lat:
        s.relay()
    for s in old + new + lat:
        s.finish()
    for s in turns + old + new + lat:
        s.done()
    for c in heads:
        c.wait()


def gather_latents(positions, seg_ids, prefix_seg, hidden, prefix_lat, gain_q, gain_kv, w_dq, w_dkv_t, w_uq, w_ukv):
    depth, q_width = w_dq.shape
    half = ROPE_DIM // 2
    freq = np.float32(ROPE_BASE) ** (-np.arange(half, dtype=np.float32) / np.float32(half))
    freq = np.tile(freq, 128 // half)[None, :].astype(np.float32)
    vmem = pl.BlockSpec(memory_space=pltpu.VMEM)
    hbm = pl.BlockSpec(memory_space=pl.ANY)
    return pl.pallas_call(
        gather_kernel,
        name="gather_latents",
        out_shape=(
            pltpu.VMEM((2, RING, RING, RING, 2, ROWS, KV_WIDTH), jnp.bfloat16),
            pltpu.VMEM((RING, RING, 2, ROWS, q_width), jnp.bfloat16),
            pltpu.VMEM((RING, RING, 2, ROWS, 128), jnp.float32),
            pltpu.VMEM((q_width, HEADS_DEV * QK_DIM), jnp.bfloat16),
            pltpu.VMEM((KV_LAT, HEADS_DEV * KV_HEAD), jnp.bfloat16),
        ),
        in_specs=[hbm] * 12,
        out_specs=(vmem,) * 5,
        scratch_shapes=[
            pltpu.SMEM((ROWS,), jnp.int32),
            pltpu.SMEM((ROWS,), jnp.int32),
            pltpu.SMEM((ROWS,), jnp.int32),
            pltpu.VMEM(hidden.shape, jnp.bfloat16),
            pltpu.VMEM(prefix_lat.shape, jnp.bfloat16),
            pltpu.VMEM(freq.shape, jnp.float32),
            pltpu.VMEM(gain_q.shape, jnp.bfloat16),
            pltpu.VMEM(gain_kv.shape, jnp.bfloat16),
            pltpu.SemaphoreType.DMA((8,)),
            pltpu.SemaphoreType.DMA((2,)),
            pltpu.VMEM((Q_SLOTS, depth // Q_CHUNKS, q_width), jnp.bfloat16),
            pltpu.VMEM((META, depth), jnp.bfloat16),
            pltpu.SemaphoreType.DMA((Q_CHUNKS,)),
            pltpu.SemaphoreType.DMA((len(KV_CHUNKS),)),
            pltpu.SemaphoreType.DMA((9, 3, 4)),
            pltpu.SemaphoreType.DMA((9, 3, 4)),
            pltpu.SemaphoreType.DMA((9, 4)),
            pltpu.SemaphoreType.DMA((9, 4)),
        ],
        compiler_params=pltpu.CompilerParams(collective_id=0, has_side_effects=True, vmem_limit_bytes=VMEM_LIMIT),
    )(*map(far, (positions, seg_ids, prefix_seg, hidden, prefix_lat, jnp.asarray(freq), gain_q, gain_kv, w_dq, w_dkv_t, w_uq, w_ukv)))


def sender(z, y, x, s):
    return lax.rem(y + RING - s // RING, RING) * RING + lax.rem(x + RING - lax.rem(s, RING), RING)


def attend_kernel(
    cs, cq, kv, wuq, wukv, wo_hbm, out, *refs,
):
    w_ahead, (wk, wvt, q_all, m_all, l_all, acc, w_sem) = refs[:W_AHEAD], refs[W_AHEAD:]
    z, y, x, core = place()
    loads = []
    depth = w_ahead[0].shape[0]
    for s in range(W_AHEAD):
        row = pl.multiple_of((core * (RING * RING) + sender(z, y, x, s)) * depth, depth)
        loads.append(pltpu.make_async_copy(wo_hbm.at[pl.ds(row, depth)], w_ahead[s], w_sem.at[s]))
    for c in loads:
        c.start()
    total = kv.shape[0] // 2
    tokens = cq.shape[0]

    def first_rows(sec):
        flags = kv[pl.ds(sec * total, total), pl.ds(KV_LAT, 128)].astype(jnp.float32)
        lane = lax.broadcasted_iota(jnp.int32, (1, 128), 1)
        return jnp.sum(jnp.where(lane == ROPE_DIM, jnp.sum(flags, axis=0, keepdims=True), 0.0)).astype(jnp.int32)

    p0, n0 = first_rows(0), first_rows(1)
    first = z * tokens
    has0, has1 = first < n0, first + tokens > n0
    old_from = jnp.where(has0, 0, p0) // KEY_BLOCK
    old_n = (jnp.where(has1, total, p0) + KEY_BLOCK - 1) // KEY_BLOCK - old_from
    new_from = (total + jnp.where(has0, 0, n0)) // KEY_BLOCK
    new_n = (total + first) // KEY_BLOCK - new_from

    token = first + lax.broadcasted_iota(jnp.int32, (SPARE, tokens), 1)
    lane = lax.broadcasted_iota(jnp.int32, (SPARE, tokens), 0)
    gate = jnp.where(lane == jnp.where(token >= n0, 0, 1), NEG_BIG, 0.0)

    for h in range(HEADS_DEV):
        at = h * KV_HEAD
        wk[:, h * 128 : h * 128 + 128] = wukv[:, at : at + NOPE_DIM]
        wvt[h * 128 : h * 128 + 128, :] = wukv[:, at + NOPE_DIM : at + KV_HEAD].T
    half = ROPE_DIM // 2
    turns = cs[...].T
    cos_t, sin_t = turns[:half], turns[3 * half :]
    q = jnp.dot(cq[...], wuq[...], preferred_element_type=jnp.float32).T
    for h in range(HEADS_DEV):
        at = h * QK_DIM
        low, high = q[at + NOPE_DIM : at + NOPE_DIM + half], q[at + NOPE_DIM + half : at + QK_DIM]
        rope = [low * cos_t - high * sin_t, high * cos_t + low * sin_t]
        q_all[h] = jnp.concatenate([q[at : at + NOPE_DIM]] + rope + [gate], axis=0).astype(jnp.bfloat16)
    scale = QK_DIM ** -0.5 * LOG2E
    nt = (((1,), (1,)), ((), ()))

    def block_of(row, size, start):
        latent = kv[pl.ds(row, size), :KV_LAT]
        tail = kv[pl.ds(row, size), KV_LAT:]
        k_all = jnp.dot(latent, wk[...], preferred_element_type=jnp.float32).astype(jnp.bfloat16)
        vt = lax.dot_general(wvt[...], latent, nt, preferred_element_type=jnp.float32).astype(jnp.bfloat16)

        def score(h):
            k = jnp.concatenate([k_all[:, h * 128 : h * 128 + 128], tail], axis=1)
            return jnp.dot(k, q_all[h], preferred_element_type=jnp.float32)

        ahead = score(0)
        for h in range(HEADS_DEV):
            s = ahead
            if h + 1 < HEADS_DEV:
                ahead = score(h + 1)
            v = vt[h * 128 : h * 128 + 128, :]
            if start:
                causal = lax.broadcasted_iota(jnp.int32, s.shape, 0) <= lax.broadcasted_iota(jnp.int32, s.shape, 1)
                s = jnp.where(causal, s, NEG_BIG)
                m_new = jnp.max(s, axis=0, keepdims=True)
                p = jnp.exp2((s - m_new) * scale)
                l_all[h] = jnp.sum(p, axis=0, keepdims=True)
                acc[h] = jnp.dot(v, p.astype(jnp.bfloat16), preferred_element_type=jnp.float32)
            else:
                m_old = m_all[h]
                m_new = jnp.maximum(m_old, jnp.max(s, axis=0, keepdims=True))
                p = jnp.exp2((s - m_new) * scale)
                fade = jnp.exp2((m_old - m_new) * scale)
                l_all[h] = l_all[h] * fade + jnp.sum(p, axis=0, keepdims=True)
                acc[h] = acc[h] * fade + jnp.dot(v, p.astype(jnp.bfloat16), preferred_element_type=jnp.float32)
            m_all[h] = m_new

    block_of(pl.multiple_of(total + first, tokens), tokens, True)

    def body(i, carry):
        row = jnp.where(i < old_n, old_from + i, new_from + i - old_n) * KEY_BLOCK
        block_of(pl.multiple_of(row, KEY_BLOCK), KEY_BLOCK, False)
        return carry

    lax.fori_loop(0, old_n + new_n, body, 0)
    for h in range(HEADS_DEV):
        out[:, h * 128 : h * 128 + 128] = (acc[h] / l_all[h]).T.astype(jnp.bfloat16)
    for c in loads:
        c.wait()


def attend(cs, cq, kv, wuq, wukv, w_o):
    tokens = cq.shape[0]
    hbm = pl.BlockSpec(memory_space=pl.ANY)
    vmem = pl.BlockSpec(memory_space=pltpu.VMEM)
    return pl.pallas_call(
        attend_kernel,
        name="attend",
        out_shape=(
            pltpu.VMEM((tokens, HEADS_DEV * V_DIM), jnp.bfloat16),
        ) + (pltpu.VMEM((HEADS_DEV * V_DIM, w_o.shape[1]), jnp.bfloat16),) * W_AHEAD,
        in_specs=[vmem] * 5 + [hbm],
        out_specs=(vmem,) * (1 + W_AHEAD),
        scratch_shapes=[
            pltpu.VMEM((KV_LAT, HEADS_DEV * NOPE_DIM), jnp.bfloat16),
            pltpu.VMEM((HEADS_DEV * V_DIM, KV_LAT), jnp.bfloat16),
            pltpu.VMEM((HEADS_DEV, 256, tokens), jnp.bfloat16),
            pltpu.VMEM((HEADS_DEV, 1, tokens), jnp.float32),
            pltpu.VMEM((HEADS_DEV, 1, tokens), jnp.float32),
            pltpu.VMEM((HEADS_DEV, V_DIM, tokens), jnp.float32),
            pltpu.SemaphoreType.DMA((W_AHEAD,)),
        ],
        compiler_params=pltpu.CompilerParams(vmem_limit_bytes=VMEM_LIMIT),
    )(cs, cq, kv, wuq, wukv, far(w_o))


def project_kernel(o_in, *refs):
    w_ahead, (wo_hbm, y_out, o_buf, w_buf, acc, other, w_sem, send_sem, recv_sem, swap_sem) = refs[:W_AHEAD], refs[W_AHEAD:]
    z, y, x, core = place()
    chip = y * RING + x
    pairs = RING * RING
    step = w_buf.shape[1]
    depth = 2 * step
    base = core * (pairs * depth)

    def load(i):
        row = pl.multiple_of(base + sender(z, y, x, W_AHEAD + i // 2) * depth + lax.rem(i, 2) * step, step)
        return pltpu.make_async_copy(wo_hbm.at[pl.ds(row, step)], w_buf.at[lax.rem(i, W_SLOTS)], w_sem.at[lax.rem(i, W_SLOTS)])

    for i in range(W_SLOTS):
        load(i).start()
    partner = index_of(z, y, x, 1 - core)
    spots = [(lax.rem(y + s // RING, RING), lax.rem(x + s % RING, RING)) for s in range(pairs)]
    all_here = greet([partner] + [index_of(z, py, px, core) for py, px in spots[1:]])
    all_here()
    sent = []
    for s in range(1, pairs):
        py, px = spots[s]
        row = pl.multiple_of((py * RING + px) * 2 * ROWS, 2 * ROWS)
        c = pltpu.make_async_remote_copy(
            src_ref=o_in.at[pl.ds(row, 2 * ROWS)], dst_ref=o_buf.at[chip], send_sem=send_sem.at[s], recv_sem=recv_sem.at[s],
            device_id={"sp": index_of(z, py, px, core)}, device_id_type=MESH,
        )
        c.start()
        sent.append(c)
    acc[...] = jnp.zeros(acc.shape, jnp.float32)
    cols = 1024

    def add(rows, w):
        for n in range(acc.shape[1] // cols):
            at = slice(n * cols, n * cols + cols)
            acc[:, at] += jnp.dot(rows, w[:, at], preferred_element_type=jnp.float32)

    def arrive(s):
        got = o_buf.at[sender(z, y, x, s)]
        pltpu.make_async_remote_copy(src_ref=got, dst_ref=got, send_sem=send_sem.at[s], recv_sem=recv_sem.at[s], device_id={"sp": partner}, device_id_type=MESH).wait_recv()

    o_buf[chip] = o_in[pl.ds(pl.multiple_of(chip * 2 * ROWS, 2 * ROWS), 2 * ROWS), :]

    def streamed(s, carry):
        arrive(s)
        for part in range(2):
            i = 2 * (s - W_AHEAD) + part
            load(i).wait()
            add(o_buf[sender(z, y, x, s), :, part * step : (part + 1) * step], w_buf.at[lax.rem(i, W_SLOTS)])

            @pl.when(i + W_SLOTS < 2 * (pairs - W_AHEAD))
            def _():
                load(i + W_SLOTS).start()

        return carry

    for s in range(W_AHEAD):
        if s:
            arrive(s)
        add(o_buf[sender(z, y, x, s)], w_ahead[s])
    lax.fori_loop(W_AHEAD, pairs, streamed, 0)
    theirs = acc.at[pl.ds(pl.multiple_of((1 - core) * ROWS, ROWS), ROWS)]
    c = pltpu.make_async_remote_copy(src_ref=theirs, dst_ref=other, send_sem=swap_sem.at[0], recv_sem=swap_sem.at[1], device_id={"sp": partner}, device_id_type=MESH)
    c.start()
    for k in sent:
        k.wait_send()
    c.wait()
    y_out[...] = (acc[pl.ds(pl.multiple_of(core * ROWS, ROWS), ROWS), :] + other[...]).astype(y_out.dtype)


def project(heads, w_ahead, w_o):
    width = w_o.shape[1]
    depth = heads.shape[1]
    return pl.pallas_call(
        project_kernel,
        name="project",
        out_shape=pltpu.VMEM((ROWS, width), jnp.bfloat16),
        in_specs=[pl.BlockSpec(memory_space=pltpu.VMEM)] * (1 + W_AHEAD) + [pl.BlockSpec(memory_space=pl.ANY)],
        out_specs=pl.BlockSpec(memory_space=pltpu.VMEM),
        scratch_shapes=[
            pltpu.VMEM((RING * RING, 2 * ROWS, depth), jnp.bfloat16),
            pltpu.VMEM((W_SLOTS, depth // 2, width), jnp.bfloat16),
            pltpu.VMEM((2 * ROWS, width), jnp.float32),
            pltpu.VMEM((ROWS, width), jnp.float32),
            pltpu.SemaphoreType.DMA((W_SLOTS,)),
            pltpu.SemaphoreType.DMA((RING * RING,)),
            pltpu.SemaphoreType.DMA((RING * RING,)),
            pltpu.SemaphoreType.DMA((2,)),
        ],
        compiler_params=pltpu.CompilerParams(collective_id=1, has_side_effects=True, vmem_limit_bytes=24 * 1024 * 1024),
    )(heads, *w_ahead, far(w_o))


def solution(mesh):
    tok_spec = P(("dp", "sp"), None)
    vec_spec = P(("dp", "sp"))
    mat_spec = P(None, None)
    gain_spec = P(None)

    def device_step(hidden, seg_ids, positions, prefix_lat, prefix_seg, w_dq, gain_q, w_uq, w_dkv, gain_kv, w_ukv, w_o):
        kv, cq, cs, wuq, wukv = gather_latents(positions, seg_ids, prefix_seg, hidden, prefix_lat, gain_q, gain_kv, w_dq, w_dkv.T, w_uq, w_ukv)
        heads, *w_ahead = attend(*map(near, (cs.reshape(-1, 128), cq.reshape(-1, cq.shape[-1]), kv.reshape(-1, KV_WIDTH), wuq, wukv)), w_o)
        return project(near(heads), tuple(map(near, w_ahead)), w_o)

    return jax.shard_map(
        device_step,
        mesh=mesh,
        in_specs=(tok_spec, vec_spec, vec_spec, tok_spec, vec_spec, mat_spec, gain_spec, mat_spec, mat_spec, gain_spec, mat_spec, mat_spec),
        out_specs=tok_spec,
        check_vma=False,
    )
```

```python
import jax
import jax.numpy as jnp
import numpy as np
from jax import lax
from jax.experimental import pallas as pl
from jax.experimental.pallas import tpu as pltpu
from jax.sharding import PartitionSpec as P

MESH = pl.DeviceIdType.MESH
KV_LAT = 512
ROPE_DIM = 64
NOPE_DIM = 128
V_DIM = 128
QK_DIM = NOPE_DIM + ROPE_DIM
KV_HEAD = NOPE_DIM + V_DIM
EPS = 1e-6
ROPE_BASE = 10000.0
NEG_BIG = -1e30
LOG2E = 1.4426950408889634
RING = 4
ROWS = 16
PLANE_TOKENS = 512
HEADS_DEV = 4
KV_WIDTH = 640
META = KV_LAT + ROPE_DIM
SPARE = KV_WIDTH - META
KEY_BLOCK = 512
W_AHEAD = 6
W_FIRST = 4
W_SLOTS = 10
Q_FLIGHT = 4
Q_SLOTS = 5
VMEM_LIMIT = 13 * 1024 * 1024 + 256 * 1024
Q_CHUNKS = 8
KV_CHUNKS = ((0, 256), (256, 256), (512, 64))


def near(array):
    return pltpu.with_memory_space_constraint(array, pltpu.VMEM)


def far(array):
    return pltpu.with_memory_space_constraint(array, pltpu.HBM)


def place():
    me = lax.axis_index("sp")
    core = lax.rem(me, 2)
    x = lax.rem(me // 2, RING)
    y = lax.rem(me // 8, RING)
    z = me // 32
    return z, y, x, core


def index_of(z, y, x, core):
    return ((z * RING + y) * RING + x) * 2 + core


def greet(peers):
    barrier = pltpu.get_barrier_semaphore()
    for peer in peers:
        pl.semaphore_signal(barrier, inc=1, device_id={"sp": peer}, device_id_type=MESH)
    return lambda: pl.semaphore_wait(barrier, len(peers))


class Stream:
    def __init__(self, slot, ref, axes, order, lanes, sems, lead=False):
        self.lead = lead
        self.slot, self.ref, self.axes, self.order, self.lanes = slot, ref, axes, order, lanes
        self.send_sem, self.recv_sem, self.swap_send, self.swap_recv = sems
        z, y, x, self.core = place()
        self.at = (z, y, x)
        self.sent = []

    def view(self, full, core, moved=None, half=None):
        index = []
        for axis in self.axes:
            if axis in full:
                both = half is None or axis != full[0]
                index.append(pl.ds(0, RING) if both else pl.ds(half * (RING // 2), RING // 2))
            elif moved is not None and moved[0] == axis:
                index.append(moved[1])
            else:
                index.append(self.at[axis])
        index = [core] + index if self.lead else index + [core]
        return self.ref.at[tuple(index) + (slice(None), self.lanes)]

    def back(self, axis, off):
        return lax.rem(self.at[axis] + RING - off, RING)

    def ahead(self, axis, off):
        to = list(self.at)
        to[axis] = lax.rem(self.at[axis] + off, RING)
        return index_of(*to, self.core)

    def copy(self, part, phase, slot, device):
        return pltpu.make_async_remote_copy(
            src_ref=part, dst_ref=part, send_sem=self.send_sem.at[self.slot, phase, slot], recv_sem=self.recv_sem.at[self.slot, phase, slot],
            device_id={"sp": device}, device_id_type=MESH,
        )

    def push(self, part, phase, slot, device):
        c = self.copy(part, phase, slot, device)
        c.start()
        self.sent.append(c)

    def swap_copy(self, off, core):
        part = self.view(self.order[:-1], core, (self.order[-1], self.back(self.order[-1], off)))
        return pltpu.make_async_remote_copy(
            src_ref=part, dst_ref=part, send_sem=self.swap_send.at[self.slot, off], recv_sem=self.swap_recv.at[self.slot, off],
            device_id={"sp": index_of(*self.at, 1 - self.core)}, device_id_type=MESH,
        )

    def swap(self, off):
        c = self.swap_copy(off, self.core)
        c.start()
        self.sent.append(c)

    def send(self, phase):
        last = phase == len(self.order) - 1
        mine = self.view(self.order[:phase], self.core)
        for off in (1, 3) if last else (1, 3, 2):
            self.push(mine, phase, off - 1, self.ahead(self.order[phase], off))
        if last:
            self.swap(0)

    def wait(self, phase, off):
        axis = self.order[phase]
        got = self.view(self.order[:phase], self.core, (axis, self.back(axis, off)))
        self.copy(got, phase, off - 1, self.ahead(axis, 1)).wait_recv()

    def step(self, phase):
        for off in (1, 3, 2):
            self.wait(phase - 1, off)
        self.send(phase)

    def relay(self):
        last = len(self.order) - 1
        axis = self.order[last]
        for off, half, slot in ((1, 0, 1), (3, 1, 3)):
            self.wait(last, off)
            part = self.view(self.order[:last], self.core, (axis, self.back(axis, off)), half)
            self.push(part, last, slot, self.ahead(axis, off))
            self.swap(off)

    def finish(self):
        last = len(self.order) - 1
        axis = self.order[last]
        for half, slot in ((0, 1), (1, 3)):
            part = self.view(self.order[:last], self.core, (axis, self.back(axis, 2)), half)
            self.copy(part, last, slot, self.ahead(axis, 1)).wait_recv()
        self.swap(2)

    def done(self):
        for off in (0, 1, 3, 2):
            self.swap_copy(off, 1 - self.core).wait_recv()
        for c in self.sent:
            c.wait_send()


def rms_norm(values, gain):
    inv_rms = lax.rsqrt(jnp.mean(values * values, axis=-1, keepdims=True) + EPS)
    return values * inv_rms * gain


def turn(values, cos_sin):
    half = ROPE_DIM // 2
    swapped = jnp.concatenate([values[:, half:], values[:, :half]], axis=1)
    return values * cos_sin[:, :ROPE_DIM] + swapped * cos_sin[:, ROPE_DIM:]


def rows_of(scalars, width):
    row = lax.broadcasted_iota(jnp.int32, (ROWS, width), 0)
    values = jnp.zeros((ROWS, width), jnp.int32)
    for r in range(ROWS):
        values = jnp.where(row == r, scalars[r], values)
    return values


def prompt_flags(seg):
    values = rows_of(seg, SPARE)
    lane = lax.broadcasted_iota(jnp.int32, values.shape, 1)
    return ((lane < 2) & (lane == values)).astype(jnp.float32).astype(jnp.bfloat16)


def gather_kernel(
    pos_hbm, seg_hbm, old_seg_hbm, hid_hbm, old_lat_hbm, freq_hbm, gain_q_hbm, gain_kv_hbm, wdq_hbm, wdkv_hbm, wuq_hbm, wukv_hbm,
    kv_buf, cq_buf, cs_buf, wuq, wukv,
    pos, seg, old_seg, both, squares, pair_sem, old_lat, freq, gain_q, gain_kv, small_sem, head_sem, wq_buf, wkv_buf, wq_sem, wkv_sem, send_sem, recv_sem, swap_send, swap_recv,
):
    z, y, x, core = place()
    depth = hid_hbm.shape[1]
    q_step = depth // Q_CHUNKS
    q_half = wq_buf.shape[2]
    kv_loads = [pltpu.make_async_copy(wdkv_hbm.at[pl.ds(at, n)], wkv_buf.at[pl.ds(at, n)], wkv_sem.at[k]) for k, (at, n) in enumerate(KV_CHUNKS)]
    q_loads = [pltpu.make_async_copy(wdq_hbm.at[pl.ds(k * q_step, q_step), pl.ds(pl.multiple_of(core * q_half, 128), q_half)], wq_buf.at[k % Q_SLOTS], wq_sem.at[k]) for k in range(Q_CHUNKS)]
    pairs = (
        (pos_hbm, pos), (old_seg_hbm, old_seg), (old_lat_hbm, old_lat), (freq_hbm, freq),
        (seg_hbm, seg), (hid_hbm, both.at[core]), (gain_kv_hbm, gain_kv), (gain_q_hbm, gain_q),
    )
    block = core * (RING * RING) + y * RING + x
    heads = [
        pltpu.make_async_copy(src.at[:, pl.ds(pl.multiple_of(block * dst.shape[1], 128), dst.shape[1])], dst, head_sem.at[k])
        for k, (src, dst) in enumerate(((wuq_hbm, wuq), (wukv_hbm, wukv)))
    ]
    small = [pltpu.make_async_copy(src, dst, small_sem.at[k]) for k, (src, dst) in enumerate(pairs)]
    for c in small + kv_loads:
        c.start()
    peers = [index_of(z, y, x, 1 - core)]
    for off in (1, 2, 3):
        peers.append(index_of(lax.rem(z + off, RING), y, x, core))
        peers.append(index_of(z, lax.rem(y + off, RING), x, core))
        peers.append(index_of(z, y, lax.rem(x + off, RING), core))
    all_here = greet(peers)
    for c in small:
        c.wait()
    for c in q_loads[:Q_FLIGHT]:
        c.start()

    kv_buf[0, z, y, x, core] = jnp.concatenate([old_lat[...], prompt_flags(old_seg)], axis=1)
    angles = rows_of(pos, 128).astype(jnp.float32) * freq[...]
    lane = lax.broadcasted_iota(jnp.int32, angles.shape, 1)
    sines = jnp.sin(angles)
    cs = jnp.where(lane < ROPE_DIM, jnp.cos(angles), jnp.where(lane < ROPE_DIM + ROPE_DIM // 2, -sines, sines))
    cs_buf[y, x, core] = cs

    all_here()
    partner = index_of(z, y, x, 1 - core)

    def to_partner(ref, k):
        return pltpu.make_async_remote_copy(
            src_ref=ref.at[core], dst_ref=ref.at[core], send_sem=pair_sem.at[k, 0], recv_sem=pair_sem.at[k, 1], device_id={"sp": partner}, device_id_type=MESH
        )

    def from_partner(ref, k):
        got = ref.at[1 - core]
        pltpu.make_async_remote_copy(
            src_ref=got, dst_ref=got, send_sem=pair_sem.at[k, 0], recv_sem=pair_sem.at[k, 1], device_id={"sp": partner}, device_id_type=MESH
        ).wait_recv()

    give = to_partner(both, 0)
    give.start()
    hid = both[core]

    sems = (send_sem, recv_sem, swap_send, swap_recv)
    lanes = (pl.ds(0, 256), pl.ds(256, 256), pl.ds(512, 128))
    space = (0, 1, 2)
    plane = (1, 2)
    to_z, to_y, to_x = (2, 1, 0), (0, 2, 1), (1, 0, 2)
    old = [Stream(i, kv_buf.at[0], space, (to_z, to_x, to_y)[i], lanes[i], sems) for i in range(3)]
    new = [Stream(3 + i, kv_buf.at[1], space, (to_z, to_y, to_x)[i], lanes[i], sems) for i in range(3)]
    half = q_half // 2
    lat = [Stream(6, cq_buf, plane, (2, 1), pl.ds(0, half), sems, True), Stream(7, cq_buf, plane, (1, 2), pl.ds(half, half), sems, True)]
    turns = [Stream(8, cs_buf, plane, (2, 1), pl.ds(0, 128), sems)]
    for s in old + turns:
        s.send(0)

    nt = (((1,), (1,)), ((), ()))
    down = []
    for k, (at, n) in enumerate(KV_CHUNKS):
        kv_loads[k].wait()
        down.append(lax.dot_general(hid, wkv_buf[at : at + n, :], nt, preferred_element_type=jnp.float32))
    kv_lat = rms_norm(jnp.concatenate(down[:-1], axis=1), gain_kv[...].astype(jnp.float32).reshape(1, -1)).astype(jnp.bfloat16)
    key_rope = turn(down[-1], cs).astype(jnp.bfloat16)
    kv_buf[1, z, y, x, core] = jnp.concatenate([kv_lat, key_rope, prompt_flags(seg)], axis=1)
    for s in new:
        s.send(0)

    from_partner(both, 0)
    q_lat = jnp.zeros((2 * ROWS, q_half), jnp.float32)
    for k in range(Q_CHUNKS):
        q_loads[k].wait()
        if k + Q_FLIGHT < Q_CHUNKS:
            q_loads[k + Q_FLIGHT].start()
        elif k + Q_FLIGHT == Q_CHUNKS:
            for c in heads:
                c.start()
        part = pl.ds(k * q_step, q_step)
        q_lat = q_lat + jnp.dot(both[:, :, part].reshape(2 * ROWS, q_step), wq_buf[k % Q_SLOTS], preferred_element_type=jnp.float32)
        if k == 3:
            for s in old + turns:
                s.step(1)
        if k == 6:
            for s in new:
                s.step(1)
    squares[core] = jnp.broadcast_to(jnp.sum(q_lat * q_lat, axis=1, keepdims=True), squares.shape[1:])
    share = to_partner(squares, 1)
    share.start()
    gains = gain_q[...].astype(jnp.float32).reshape(1, -1)
    gains = jnp.where(core == 0, gains[:, :q_half], gains[:, q_half:])
    from_partner(squares, 1)
    mean = (squares[0, :, :1] + squares[1, :, :1]) / (2 * q_half)
    cq_buf[core, y, x] = (q_lat * lax.rsqrt(mean + EPS) * gains).astype(jnp.bfloat16)
    for s in lat:
        s.send(0)
    for s in old:
        s.step(2)
    for s in turns:
        s.relay()
    for s in new:
        s.step(2)
    for s in lat:
        s.step(1)
    for s in turns:
        s.finish()
    for s in old + new + lat:
        s.relay()
    for s in old + new + lat:
        s.finish()
    for s in turns + old + new + lat:
        s.done()
    for c in heads:
        c.wait()
    give.wait_send()
    share.wait_send()


def gather_latents(positions, seg_ids, prefix_seg, hidden, prefix_lat, gain_q, gain_kv, w_dq, w_dkv_t, w_uq, w_ukv):
    depth, q_width = w_dq.shape
    half = ROPE_DIM // 2
    freq = np.float32(ROPE_BASE) ** (-np.arange(half, dtype=np.float32) / np.float32(half))
    freq = np.tile(freq, 128 // half)[None, :].astype(np.float32)
    vmem = pl.BlockSpec(memory_space=pltpu.VMEM)
    hbm = pl.BlockSpec(memory_space=pl.ANY)
    return pl.pallas_call(
        gather_kernel,
        name="gather_latents",
        out_shape=(
            pltpu.VMEM((2, RING, RING, RING, 2, ROWS, KV_WIDTH), jnp.bfloat16),
            pltpu.VMEM((2, RING, RING, 2 * ROWS, q_width // 2), jnp.bfloat16),
            pltpu.VMEM((RING, RING, 2, ROWS, 128), jnp.float32),
            pltpu.VMEM((q_width, HEADS_DEV * QK_DIM), jnp.bfloat16),
            pltpu.VMEM((KV_LAT, HEADS_DEV * KV_HEAD), jnp.bfloat16),
        ),
        in_specs=[hbm] * 12,
        out_specs=(vmem,) * 5,
        scratch_shapes=[
            pltpu.SMEM((ROWS,), jnp.int32),
            pltpu.SMEM((ROWS,), jnp.int32),
            pltpu.SMEM((ROWS,), jnp.int32),
            pltpu.VMEM((2,) + hidden.shape, jnp.bfloat16),
            pltpu.VMEM((2, 2 * ROWS, 128), jnp.float32),
            pltpu.SemaphoreType.DMA((2, 2)),
            pltpu.VMEM(prefix_lat.shape, jnp.bfloat16),
            pltpu.VMEM(freq.shape, jnp.float32),
            pltpu.VMEM(gain_q.shape, jnp.bfloat16),
            pltpu.VMEM(gain_kv.shape, jnp.bfloat16),
            pltpu.SemaphoreType.DMA((8,)),
            pltpu.SemaphoreType.DMA((2,)),
            pltpu.VMEM((Q_SLOTS, depth // Q_CHUNKS, q_width // 2), jnp.bfloat16),
            pltpu.VMEM((META, depth), jnp.bfloat16),
            pltpu.SemaphoreType.DMA((Q_CHUNKS,)),
            pltpu.SemaphoreType.DMA((len(KV_CHUNKS),)),
            pltpu.SemaphoreType.DMA((9, 3, 4)),
            pltpu.SemaphoreType.DMA((9, 3, 4)),
            pltpu.SemaphoreType.DMA((9, 4)),
            pltpu.SemaphoreType.DMA((9, 4)),
        ],
        compiler_params=pltpu.CompilerParams(collective_id=0, has_side_effects=True, vmem_limit_bytes=VMEM_LIMIT),
    )(*map(far, (positions, seg_ids, prefix_seg, hidden, prefix_lat, jnp.asarray(freq), gain_q, gain_kv, w_dq, w_dkv_t, w_uq, w_ukv)))


def sender(z, y, x, s):
    return lax.rem(y + RING - s // RING, RING) * RING + lax.rem(x + RING - lax.rem(s, RING), RING)


def attend_kernel(
    cs, cq, kv, wuq, wukv, wo_hbm, out, *refs,
):
    w_ahead, (wk, wvt, q_all, m_all, l_all, acc, w_sem) = refs[:W_AHEAD], refs[W_AHEAD:]
    z, y, x, core = place()
    loads = []
    depth = w_ahead[0].shape[0]
    for s in range(W_AHEAD):
        row = pl.multiple_of((core * (RING * RING) + sender(z, y, x, W_FIRST + s)) * depth, depth)
        loads.append(pltpu.make_async_copy(wo_hbm.at[pl.ds(row, depth)], w_ahead[s], w_sem.at[s]))
    for c in loads:
        c.start()
    total = kv.shape[0] // 2
    tokens = cq.shape[1]

    def first_rows(sec):
        flags = kv[pl.ds(sec * total, total), pl.ds(KV_LAT, 128)].astype(jnp.float32)
        lane = lax.broadcasted_iota(jnp.int32, (1, 128), 1)
        return jnp.sum(jnp.where(lane == ROPE_DIM, jnp.sum(flags, axis=0, keepdims=True), 0.0)).astype(jnp.int32)

    p0, n0 = first_rows(0), first_rows(1)
    first = z * tokens
    has0, has1 = first < n0, first + tokens > n0
    old_from = jnp.where(has0, 0, p0) // KEY_BLOCK
    old_n = (jnp.where(has1, total, p0) + KEY_BLOCK - 1) // KEY_BLOCK - old_from
    new_from = (total + jnp.where(has0, 0, n0)) // KEY_BLOCK
    new_n = (total + first) // KEY_BLOCK - new_from

    token = first + lax.broadcasted_iota(jnp.int32, (SPARE, tokens), 1)
    lane = lax.broadcasted_iota(jnp.int32, (SPARE, tokens), 0)
    gate = jnp.where(lane == jnp.where(token >= n0, 0, 1), NEG_BIG, 0.0)

    for h in range(HEADS_DEV):
        at = h * KV_HEAD
        wk[:, h * 128 : h * 128 + 128] = wukv[:, at : at + NOPE_DIM]
        wvt[h * 128 : h * 128 + 128, :] = wukv[:, at + NOPE_DIM : at + KV_HEAD].T
    half = ROPE_DIM // 2
    turns = cs[...].T
    cos_t, sin_t = turns[:half], turns[3 * half :]
    width = cq.shape[2]
    q = jnp.dot(cq[0], wuq[:width], preferred_element_type=jnp.float32)
    q = (q + jnp.dot(cq[1], wuq[width:], preferred_element_type=jnp.float32)).T
    for h in range(HEADS_DEV):
        at = h * QK_DIM
        low, high = q[at + NOPE_DIM : at + NOPE_DIM + half], q[at + NOPE_DIM + half : at + QK_DIM]
        rope = [low * cos_t - high * sin_t, high * cos_t + low * sin_t]
        q_all[h] = jnp.concatenate([q[at : at + NOPE_DIM]] + rope + [gate], axis=0).astype(jnp.bfloat16)
    scale = QK_DIM ** -0.5 * LOG2E
    nt = (((1,), (1,)), ((), ()))

    def block_of(row, size, start):
        latent = kv[pl.ds(row, size), :KV_LAT]
        tail = kv[pl.ds(row, size), KV_LAT:]
        k_all = jnp.dot(latent, wk[...], preferred_element_type=jnp.float32).astype(jnp.bfloat16)
        vt = lax.dot_general(wvt[...], latent, nt, preferred_element_type=jnp.float32).astype(jnp.bfloat16)

        def score(h):
            k = jnp.concatenate([k_all[:, h * 128 : h * 128 + 128], tail], axis=1)
            return jnp.dot(k, q_all[h], preferred_element_type=jnp.float32)

        ahead = score(0)
        for h in range(HEADS_DEV):
            s = ahead
            if h + 1 < HEADS_DEV:
                ahead = score(h + 1)
            v = vt[h * 128 : h * 128 + 128, :]
            if start:
                causal = lax.broadcasted_iota(jnp.int32, s.shape, 0) <= lax.broadcasted_iota(jnp.int32, s.shape, 1)
                s = jnp.where(causal, s, NEG_BIG)
                m_new = jnp.max(s, axis=0, keepdims=True)
                p = jnp.exp2((s - m_new) * scale)
                l_all[h] = jnp.sum(p, axis=0, keepdims=True)
                acc[h] = jnp.dot(v, p.astype(jnp.bfloat16), preferred_element_type=jnp.float32)
            else:
                m_old = m_all[h]
                m_new = jnp.maximum(m_old, jnp.max(s, axis=0, keepdims=True))
                p = jnp.exp2((s - m_new) * scale)
                fade = jnp.exp2((m_old - m_new) * scale)
                l_all[h] = l_all[h] * fade + jnp.sum(p, axis=0, keepdims=True)
                acc[h] = acc[h] * fade + jnp.dot(v, p.astype(jnp.bfloat16), preferred_element_type=jnp.float32)
            m_all[h] = m_new

    block_of(pl.multiple_of(total + first, tokens), tokens, True)

    def body(i, carry):
        row = jnp.where(i < old_n, old_from + i, new_from + i - old_n) * KEY_BLOCK
        block_of(pl.multiple_of(row, KEY_BLOCK), KEY_BLOCK, False)
        return carry

    lax.fori_loop(0, old_n + new_n, body, 0)
    for h in range(HEADS_DEV):
        out[:, h * 128 : h * 128 + 128] = (acc[h] / l_all[h]).T.astype(jnp.bfloat16)
    for c in loads:
        c.wait()


def attend(cs, cq, kv, wuq, wukv, w_o):
    tokens = cq.shape[1]
    hbm = pl.BlockSpec(memory_space=pl.ANY)
    vmem = pl.BlockSpec(memory_space=pltpu.VMEM)
    return pl.pallas_call(
        attend_kernel,
        name="attend",
        out_shape=(
            pltpu.VMEM((tokens, HEADS_DEV * V_DIM), jnp.bfloat16),
        ) + (pltpu.VMEM((HEADS_DEV * V_DIM, w_o.shape[1]), jnp.bfloat16),) * W_AHEAD,
        in_specs=[vmem] * 5 + [hbm],
        out_specs=(vmem,) * (1 + W_AHEAD),
        scratch_shapes=[
            pltpu.VMEM((KV_LAT, HEADS_DEV * NOPE_DIM), jnp.bfloat16),
            pltpu.VMEM((HEADS_DEV * V_DIM, KV_LAT), jnp.bfloat16),
            pltpu.VMEM((HEADS_DEV, 256, tokens), jnp.bfloat16),
            pltpu.VMEM((HEADS_DEV, 1, tokens), jnp.float32),
            pltpu.VMEM((HEADS_DEV, 1, tokens), jnp.float32),
            pltpu.VMEM((HEADS_DEV, V_DIM, tokens), jnp.float32),
            pltpu.SemaphoreType.DMA((W_AHEAD,)),
        ],
        compiler_params=pltpu.CompilerParams(vmem_limit_bytes=VMEM_LIMIT),
    )(cs, cq, kv, wuq, wukv, far(w_o))


def project_kernel(o_in, *refs):
    w_ahead, (wo_hbm, y_out, o_buf, w_buf, acc, other, w_sem, send_sem, recv_sem, swap_sem) = refs[:W_AHEAD], refs[W_AHEAD:]
    z, y, x, core = place()
    chip = y * RING + x
    pairs = RING * RING
    step = w_buf.shape[1]
    depth = 2 * step
    base = core * (pairs * depth)

    def load(i):
        s = i // 2 + jnp.where(i < 2 * W_FIRST, 0, W_AHEAD)
        row = pl.multiple_of(base + sender(z, y, x, s) * depth + lax.rem(i, 2) * step, step)
        return pltpu.make_async_copy(wo_hbm.at[pl.ds(row, step)], w_buf.at[lax.rem(i, W_SLOTS)], w_sem.at[lax.rem(i, W_SLOTS)])

    for i in range(W_SLOTS):
        load(i).start()
    partner = index_of(z, y, x, 1 - core)
    spots = [(lax.rem(y + s // RING, RING), lax.rem(x + s % RING, RING)) for s in range(pairs)]
    all_here = greet([partner] + [index_of(z, py, px, core) for py, px in spots[1:]])
    all_here()
    sent = []
    for s in range(1, pairs):
        py, px = spots[s]
        row = pl.multiple_of((py * RING + px) * 2 * ROWS, 2 * ROWS)
        c = pltpu.make_async_remote_copy(
            src_ref=o_in.at[pl.ds(row, 2 * ROWS)], dst_ref=o_buf.at[chip], send_sem=send_sem.at[s], recv_sem=recv_sem.at[s],
            device_id={"sp": index_of(z, py, px, core)}, device_id_type=MESH,
        )
        c.start()
        sent.append(c)
    acc[...] = jnp.zeros(acc.shape, jnp.float32)
    cols = 1024

    mine = pl.ds(pl.multiple_of(core * ROWS, ROWS), ROWS)
    theirs = pl.ds(pl.multiple_of((1 - core) * ROWS, ROWS), ROWS)

    def swap(n):
        return pltpu.make_async_remote_copy(
            src_ref=acc.at[theirs, pl.ds(n * cols, cols)], dst_ref=other.at[:, pl.ds(n * cols, cols)],
            send_sem=swap_sem.at[0, n], recv_sem=swap_sem.at[1, n], device_id={"sp": partner}, device_id_type=MESH,
        )

    def add(rows, w, last=False):
        for n in range(acc.shape[1] // cols):
            at = slice(n * cols, n * cols + cols)
            acc[:, at] += jnp.dot(rows, w[:, at], preferred_element_type=jnp.float32)
            if last:
                swap(n).start()

    def arrive(s):
        got = o_buf.at[sender(z, y, x, s)]
        pltpu.make_async_remote_copy(src_ref=got, dst_ref=got, send_sem=send_sem.at[s], recv_sem=recv_sem.at[s], device_id={"sp": partner}, device_id_type=MESH).wait_recv()

    o_buf[chip] = o_in[pl.ds(pl.multiple_of(chip * 2 * ROWS, 2 * ROWS), 2 * ROWS), :]

    streams = pairs - W_AHEAD

    def use(i, s, part, last=False):
        load(i).wait()
        add(o_buf[sender(z, y, x, s), :, part * step : (part + 1) * step], w_buf.at[lax.rem(i, W_SLOTS)], last)

    def streamed(k, carry):
        s = k + jnp.where(k < W_FIRST, 0, W_AHEAD)

        @pl.when(k > 0)
        def _():
            arrive(s)

        for part in range(2):
            i = 2 * k + part
            use(i, s, part)

            @pl.when(i + W_SLOTS < 2 * streams)
            def _():
                load(i + W_SLOTS).start()

        return carry

    lax.fori_loop(0, W_FIRST, streamed, 0)
    for s in range(W_AHEAD):
        arrive(W_FIRST + s)
        add(o_buf[sender(z, y, x, W_FIRST + s)], w_ahead[s])
    lax.fori_loop(W_FIRST, streams - 1, streamed, 0)
    arrive(pairs - 1)
    use(2 * streams - 2, pairs - 1, 0)
    use(2 * streams - 1, pairs - 1, 1, True)
    for k in sent:
        k.wait_send()
    for n in range(acc.shape[1] // cols):
        swap(n).wait()
    y_out[...] = (acc[mine, :] + other[...]).astype(y_out.dtype)


def project(heads, w_ahead, w_o):
    width = w_o.shape[1]
    depth = heads.shape[1]
    return pl.pallas_call(
        project_kernel,
        name="project",
        out_shape=pltpu.VMEM((ROWS, width), jnp.bfloat16),
        in_specs=[pl.BlockSpec(memory_space=pltpu.VMEM)] * (1 + W_AHEAD) + [pl.BlockSpec(memory_space=pl.ANY)],
        out_specs=pl.BlockSpec(memory_space=pltpu.VMEM),
        scratch_shapes=[
            pltpu.VMEM((RING * RING, 2 * ROWS, depth), jnp.bfloat16),
            pltpu.VMEM((W_SLOTS, depth // 2, width), jnp.bfloat16),
            pltpu.VMEM((2 * ROWS, width), jnp.float32),
            pltpu.VMEM((ROWS, width), jnp.float32),
            pltpu.SemaphoreType.DMA((W_SLOTS,)),
            pltpu.SemaphoreType.DMA((RING * RING,)),
            pltpu.SemaphoreType.DMA((RING * RING,)),
            pltpu.SemaphoreType.DMA((2, 5)),
        ],
        compiler_params=pltpu.CompilerParams(collective_id=1, has_side_effects=True, vmem_limit_bytes=27 * 1024 * 1024),
    )(heads, *w_ahead, far(w_o))


def solution(mesh):
    tok_spec = P(("dp", "sp"), None)
    vec_spec = P(("dp", "sp"))
    mat_spec = P(None, None)
    gain_spec = P(None)

    def device_step(hidden, seg_ids, positions, prefix_lat, prefix_seg, w_dq, gain_q, w_uq, w_dkv, gain_kv, w_ukv, w_o):
        kv, cq, cs, wuq, wukv = gather_latents(positions, seg_ids, prefix_seg, hidden, prefix_lat, gain_q, gain_kv, w_dq, w_dkv.T, w_uq, w_ukv)
        heads, *w_ahead = attend(*map(near, (cs.reshape(-1, 128), cq.reshape(2, -1, cq.shape[-1]), kv.reshape(-1, KV_WIDTH), wuq, wukv)), w_o)
        return project(near(heads), tuple(map(near, w_ahead)), w_o)

    return jax.shard_map(
        device_step,
        mesh=mesh,
        in_specs=(tok_spec, vec_spec, vec_spec, tok_spec, vec_spec, mat_spec, gain_spec, mat_spec, mat_spec, gain_spec, mat_spec, mat_spec),
        out_specs=tok_spec,
        check_vma=False,
    )
```
